1024 devices in a mesh: gx: 8 (over z_hi, core), gy: 16 (over z_lo, x), gz: 8 (over y).
Axes of the slice: x: 4, y: 8, z: 16 (z_hi: 4, z_lo: 4; z = z_hi * 4 + z_lo), core: 2. Of those that a mesh axis runs over, the one named last changes fastest.
Arguments:
- particle_fields: float32 [20, 8388608], P(None, ('gx', 'gy', 'gz')), may hold values from -4 to 4
- step_length: float32 [8388608], P(('gx', 'gy', 'gz')), may hold values from 0.1 to 1
- live_mask: int32 [8388608], P(('gx', 'gy', 'gz')), may hold values 0 or 1
- dest_cell: int32 [8388608], P(('gx', 'gy', 'gz')), may hold values from 0 to 511
- block_counts: int32 [1024, 6], P(('gx', 'gy', 'gz')), may hold values from 0 to 12, as said below
- block_lists: int32 [1024, 48], P(('gx', 'gy', 'gz')), may hold values from 0 to 87, as said below
Outputs:
- tile_sums: float32 [20, 524288], P(None, ('gx', 'gy', 'gz'))
The draws below stay inside these ranges and needn't reach their ends.
Inputs may be any that keep to these rules, and one draw needn't show every extreme that they name: `block_counts`: columns are directions in the order x lower, x upper, z lower, z upper, y lower, y upper; a count is at most its section's span (6, 6 or 12) and may be 0; at every section some domain receives full spans from both neighbours. `block_lists`: per domain, 6 entries toward the lower x neighbour, 6 toward the upper, then 2 * 6 for z and 24 for y in the same way; entries are block numbers of the domain's pool at that section. Entries below their direction's count are valid: valid entries of one domain over all sections are distinct, and each names an own block or an appended block that its sender filled. Other entries are arbitrary numbers within the pool.
All inputs are finite; a program needn't handle non-finite values. No bound on the sum of `live_mask` on one device may be relied on, other than what follows from the above.
Results may differ from the reference program's by a relative error of at most 0.0003.
Values sent between devices are 32-bit elements; how exact they have to be, the bound alone decides.
A program may use at most 32 MiB of HBM per device.

```python
import math
import jax
import jax.numpy as jnp

FIELDS = 20
BLOCKS = 64
CELLS = 512
CAP_X = 6
CAP_Z = 6
CAP_Y = 12
LIST_LEN = 48
PARTICLES = 8388608
N_GX = 8
N_GY = 16
N_GZ = 8


def plan_migration(key):
    shape_grid = (N_GX, N_GY, N_GZ)
    final_count = BLOCKS + 2 * (CAP_X + CAP_Z + CAP_Y)
    pool_index = jnp.arange(final_count, dtype=jnp.int32)
    eligible = jnp.broadcast_to(pool_index < BLOCKS, shape_grid + (final_count,))
    coords = jnp.meshgrid(jnp.arange(N_GX, dtype=jnp.int32), jnp.arange(N_GY, dtype=jnp.int32), jnp.arange(N_GZ, dtype=jnp.int32), indexing='ij')
    extents_grid = jnp.array(shape_grid, dtype=jnp.int32)
    size_now = BLOCKS
    count_parts = []
    list_parts = []
    for section_index, (axis_place, extent) in enumerate(((0, CAP_X), (2, CAP_Z), (1, CAP_Y))):
        section_key = jax.random.fold_in(key, 101 + section_index)
        count_key, pick_key, filler_key, target_key = jax.random.split(section_key, 4)
        rough_draw = jax.random.randint(count_key, shape_grid + (2,), 0, extent + 1, dtype=jnp.int32)
        number = rough_draw * rough_draw // extent
        target = jax.random.randint(target_key, (3,), 0, extents_grid, dtype=jnp.int32)
        step_unit = (jnp.arange(3) == axis_place).astype(jnp.int32)
        lower_site = (target - step_unit) % extents_grid
        upper_site = (target + step_unit) % extents_grid
        at_lower = (coords[0] == lower_site[0]) & (coords[1] == lower_site[1]) & (coords[2] == lower_site[2])
        at_upper = (coords[0] == upper_site[0]) & (coords[1] == upper_site[1]) & (coords[2] == upper_site[2])
        toward_lower = jnp.where(at_upper, extent, number[..., 0]).astype(jnp.int32)
        toward_upper = jnp.where(at_lower, extent, number[..., 1]).astype(jnp.int32)
        scores = jax.random.randint(pick_key, shape_grid + (final_count,), 0, 1 << 20, dtype=jnp.int32) * final_count + pool_index
        scores = jnp.where(eligible, scores, -1)
        chosen = jnp.argsort(-scores, axis=-1)[..., :2 * extent].astype(jnp.int32)
        position = jnp.arange(2 * extent) % extent
        wanted = jnp.where(jnp.arange(2 * extent) < extent, toward_lower[..., None], toward_upper[..., None])
        usable = position < wanted
        filler = jax.random.randint(filler_key, shape_grid + (2 * extent,), 0, size_now, dtype=jnp.int32)
        list_parts.append(jnp.where(usable, chosen, filler))
        count_parts.append(jnp.stack([toward_lower, toward_upper], axis=-1))
        taken_now = jnp.any((chosen[..., :, None] == pool_index) & usable[..., None], axis=-2)
        from_lower = jnp.roll(toward_upper, 1, axis=axis_place)
        from_upper = jnp.roll(toward_lower, -1, axis=axis_place)
        offset = pool_index - size_now
        landed = (offset >= 0) & (offset < extent) & (offset < from_lower[..., None]) | (offset >= extent) & (offset < 2 * extent) & (offset - extent < from_upper[..., None])
        eligible = eligible & jnp.logical_not(taken_now) | landed
        size_now = size_now + 2 * extent
    counts = jnp.concatenate(count_parts, axis=-1).reshape(N_GX * N_GY * N_GZ, 6)
    entries = jnp.concatenate(list_parts, axis=-1).reshape(N_GX * N_GY * N_GZ, 2 * (CAP_X + CAP_Z + CAP_Y))
    return (counts.astype(jnp.int32), entries.astype(jnp.int32))


def draw_block_counts(key, part):
    return plan_migration(key)[0]


def draw_block_lists(key, part):
    return plan_migration(key)[1]


def set_ends(values, stream_key, low, high):
    dims = values.shape
    place = [jax.random.randint(jax.random.fold_in(stream_key, axis), (), 0, dims[axis]) for axis in range(len(dims))]
    values = values.at[tuple(place)].set(low)
    longest = dims.index(max(dims))
    place[longest] = (place[longest] + 1) % dims[longest]
    return values.at[tuple(place)].set(high)


def levels(stream_key, dims, pieces, least, high):
    loudness, own = 1.0, jax.random.fold_in(stream_key, 6)
    for axis_at, shards_of in pieces:
        steps = jnp.exp(jax.random.uniform(jax.random.fold_in(own, axis_at), (shards_of,), jnp.float32, least / len(pieces), high / len(pieces)))
        loudness = loudness * jnp.repeat(steps, dims[axis_at] // shards_of).reshape([-1 if axis == axis_at else 1 for axis in range(len(dims))])
    return loudness


def centred(rng, shape, deviation, reach, cuts=(), kind=jnp.bfloat16):
    values = jax.random.normal(rng, shape, jnp.float32) * deviation
    if len(cuts) > 0:
        values = levels(rng, shape, cuts, -0.22, 0.18) * values
    return jnp.clip(values, min=-reach, max=reach).astype(kind)


def setup_inputs(seed: int = 0) -> dict:
    arg_keys = jax.random.split(jax.random.key(seed), 7)
    return {
        "particle_fields": centred(arg_keys[0], (FIELDS, PARTICLES), 0.25, 4.0, ((1, 1024),), jnp.float32),
        "step_length": jnp.clip(jnp.exp(math.log(1.0) - 2.3025851 * jax.random.uniform(arg_keys[1], (PARTICLES,), jnp.float32) ** levels(arg_keys[1], (PARTICLES,), ((0, 1024),), -0.2, 0.2)), 0.1, 1.0),
        "live_mask": set_ends((jax.random.randint(arg_keys[2], (PARTICLES,), 0, 4) < 3).astype(jnp.int32), jax.random.fold_in(arg_keys[2], 1), 0, 1),
        "dest_cell": set_ends(jax.random.randint(arg_keys[3], (PARTICLES,), 0, CELLS), jax.random.fold_in(arg_keys[3], 1), 0, CELLS - 1).astype(jnp.int32),
        "block_counts": draw_block_counts(jax.random.fold_in(arg_keys[6], 71), 0),
        "block_lists": draw_block_lists(jax.random.fold_in(arg_keys[6], 71), 0),
    }


def leave_section(holding, chosen, number, axis_place):
    extent = chosen.shape[-1] // 2
    index_full = jnp.broadcast_to(chosen.astype(jnp.int32)[None, :, :, :, :, None], holding.shape[:4] + (2 * extent, 128))
    picked = jnp.take_along_axis(holding, index_full, axis=4)
    position = jnp.arange(2 * extent) % extent
    wanted = jnp.where(jnp.arange(2 * extent) < extent, number[..., 0:1], number[..., 1:2])
    usable = (position < wanted).astype(jnp.float32)
    outgoing = picked * usable[None, :, :, :, :, None]
    from_lower = jnp.roll(outgoing[:, :, :, :, extent:], 1, axis=axis_place + 1)
    from_upper = jnp.roll(outgoing[:, :, :, :, :extent], -1, axis=axis_place + 1)
    return jnp.concatenate([holding, from_lower, from_upper], axis=4)


def reference(particle_fields, step_length, live_mask, dest_cell, block_counts, block_lists):
    advanced = particle_fields[0:3] + step_length[None, :] * particle_fields[3:6]
    carried = jnp.concatenate([advanced, particle_fields[3:], live_mask.astype(jnp.float32)[None, :], dest_cell.astype(jnp.float32)[None, :]], axis=0)
    row_count = FIELDS + 2
    domain_count = N_GX * N_GY * N_GZ
    holding = carried.reshape(row_count, N_GX, N_GY, N_GZ, BLOCKS, 128)
    number = block_counts.reshape(N_GX, N_GY, N_GZ, 6)
    entries = block_lists.reshape(N_GX, N_GY, N_GZ, LIST_LEN)
    first_end = 2 * CAP_X
    second_end = first_end + 2 * CAP_Z
    holding = leave_section(holding, entries[..., :first_end], number[..., 0:2], 0)
    holding = leave_section(holding, entries[..., first_end:second_end], number[..., 2:4], 2)
    before_count = holding.shape[4]
    holding = leave_section(holding, entries[..., second_end:], number[..., 4:6], 1)
    spans = (CAP_X, CAP_X, CAP_Z, CAP_Z, CAP_Y, CAP_Y)
    limits = [jnp.broadcast_to(number[..., column:column + 1], (N_GX, N_GY, N_GZ, extent)) for column, extent in enumerate(spans)]
    wanted = jnp.concatenate(limits, axis=-1)
    position = jnp.concatenate([jnp.arange(extent) for extent in spans])
    listed = (entries[..., :, None] == jnp.arange(before_count)[None, None, None, None, :]) & (position < wanted)[..., None]
    keep_before = 1.0 - jnp.any(listed, axis=3).astype(jnp.float32)
    keep_block = jnp.concatenate([keep_before, jnp.ones((N_GX, N_GY, N_GZ, holding.shape[4] - before_count), jnp.float32)], axis=-1)
    weights = holding[FIELDS] * keep_block[..., None]
    domain = jnp.arange(domain_count, dtype=jnp.int32).reshape(N_GX, N_GY, N_GZ, 1, 1)
    segment = (domain * CELLS + holding[FIELDS + 1].astype(jnp.int32)).reshape(-1)
    columns = []
    for field_index in range(FIELDS):
        columns.append(jax.ops.segment_sum((holding[field_index] * weights).reshape(-1), segment, num_segments=domain_count * CELLS))
    return jnp.stack(columns, axis=0)
```

```python
import functools

import jax
import jax.numpy as jnp
from jax import lax
from jax.experimental import pallas as pl
from jax.experimental.pallas import tpu as pltpu
from jax.sharding import PartitionSpec as P

MESH = pl.DeviceIdType.MESH
FIELDS = 20
BLOCKS = 64
CELLS = 512
CAP_X = 6
CAP_Z = 6
CAP_Y = 12
LIST_LEN = 48
ROWS = 24
GROUP = 8
AXES = ("gx", "gy", "gz")


def kernel(
    sizes,
    fields_hbm,
    step_hbm,
    live_hbm,
    cell_hbm,
    counts_hbm,
    lists_hbm,
    out_ref,
    fields,
    step,
    live,
    cell,
    counts,
    lists,
    lists_vec,
    own,
    x_send,
    x_in,
    z_send,
    z_in,
    y_send,
    y_in,
    mask,
    acc,
    load_sem,
    send_sem,
    recv_sem,
):
    def beside(axis, shift):
        n = sizes[axis]
        return {axis: lax.rem(lax.axis_index(axis) + shift + n, n)}

    barrier = pltpu.get_barrier_semaphore()
    for axis in AXES:
        for shift in (-1, 1):
            pl.semaphore_signal(
                barrier, inc=1, device_id=beside(axis, shift), device_id_type=MESH
            )

    loads = [
        pltpu.make_async_copy(counts_hbm, counts, load_sem.at[0]),
        pltpu.make_async_copy(lists_hbm, lists, load_sem.at[1]),
        pltpu.make_async_copy(lists_hbm, lists_vec, load_sem.at[2]),
        pltpu.make_async_copy(step_hbm, step, load_sem.at[3]),
        pltpu.make_async_copy(live_hbm, live, load_sem.at[4]),
        pltpu.make_async_copy(cell_hbm, cell, load_sem.at[5]),
        pltpu.make_async_copy(fields_hbm, fields, load_sem.at[6]),
    ]
    for load in loads:
        load.start()
    for load in loads:
        load.wait()

    row = lax.broadcasted_iota(jnp.int32, (8, 128), 0)

    def prepare(block, _):
        columns = pl.ds(pl.multiple_of(block * 128, 128), 128)
        one = pl.ds(block, 1)
        weight = jnp.broadcast_to(live[one, :].astype(jnp.float32), (8, 128))
        length = jnp.broadcast_to(step[one, :], (8, 128))
        place = jnp.broadcast_to(cell[one, :].astype(jnp.float32), (8, 128))
        first = fields[0:8, columns]
        moved = first + length * pltpu.roll(first, 5, 0)
        first = jnp.where(row < 3, moved, first)
        tail = jnp.where(row[0:4] == 0, place[0:4], 0.0)
        last = jnp.concatenate([fields[16:20, columns] * weight[0:4], tail], axis=0)
        own[block, 0:8, :] = first * weight
        own[block, 8:16, :] = fields[8:16, columns] * weight
        own[block, 16:24, :] = last
        return 0

    lax.fori_loop(0, BLOCKS, prepare, 0, unroll=4)

    def pick(entry, usable, arrived):
        chosen = own[jnp.clip(entry, 0, BLOCKS - 1)]
        if arrived is not None:
            other = arrived[jnp.clip(entry - BLOCKS, 0, 2 * CAP_X - 1)]
            chosen = jnp.where(entry < BLOCKS, chosen, other)
        return jnp.where(usable, chosen, 0.0)

    def gather(first, count, extent, arrived, target):
        for slot in range(2 * extent):
            entry = lists[0, first + slot]
            usable = slot % extent < counts[0, count + slot // extent]
            target[slot] = pick(entry, usable, arrived)

    def exchange(axis, at, send, arrived, extent):
        copies = []
        for k, shift in ((0, 1), (1, -1)):
            source = pl.ds(extent, extent) if shift == 1 else pl.ds(0, extent)
            target = pl.ds(0, extent) if shift == 1 else pl.ds(extent, extent)
            copy = pltpu.make_async_remote_copy(
                src_ref=send.at[source],
                dst_ref=arrived.at[target],
                send_sem=send_sem.at[at + k],
                recv_sem=recv_sem.at[at + k],
                device_id=beside(axis, shift),
                device_id_type=MESH,
            )
            copy.start()
            copies.append(copy)
        return copies

    gather(0, 0, CAP_X, None, x_send)
    pl.semaphore_wait(barrier, 6)
    x_copies = exchange("gx", 0, x_send, x_in, CAP_X)

    lane = lax.broadcasted_iota(jnp.int32, (1, LIST_LEN), 1)
    limit = jnp.zeros((1, LIST_LEN), jnp.int32)
    begin = 0
    for column, extent in enumerate((CAP_X, CAP_X, CAP_Z, CAP_Z, CAP_Y, CAP_Y)):
        inside = (lane >= begin) & (lane < begin + extent)
        limit = jnp.where(inside, counts[0, column] + begin, limit)
        begin += extent
    named = jnp.where(lane < limit, lists_vec[...], -1)
    lower = (lane >= LIST_LEN - 2 * CAP_Y) & (lane < LIST_LEN - CAP_Y)
    upper = lane >= LIST_LEN - CAP_Y
    total = BLOCKS + 2 * CAP_X + 2 * CAP_Z
    block_id = lax.broadcasted_iota(jnp.int32, (total, LIST_LEN), 0)
    for k, part in enumerate((named, jnp.where(lower, named, -1), jnp.where(upper, named, -1))):
        found = jnp.where(block_id == part, 1.0, 0.0)
        found = jnp.max(found, axis=1, keepdims=True)
        if k == 0:
            found = 1.0 - found
        mask[k] = jnp.broadcast_to(found, (total, 128))

    tile = lax.broadcasted_iota(jnp.int32, (CELLS, 128), 0).astype(jnp.float32)

    def binned(source, start, at, blocks):
        hot, values = [], ([], [], [])
        for k in range(blocks):
            block = source[start + k]
            hot.append(jnp.where(tile == block[20:21, :], 1.0, 0.0).astype(jnp.bfloat16))
            high = block.astype(jnp.bfloat16).astype(jnp.float32)
            both = jnp.concatenate([high, block - high], axis=0)
            for c in range(3):
                weight = mask[c, pl.ds(at + k, 1), :]
                values[c].append((both * weight).astype(jnp.bfloat16))
        left = jnp.concatenate([jnp.concatenate(v, axis=1) for v in values], axis=0)
        right = jnp.concatenate(hot, axis=1)
        return lax.dot_general(
            left, right, (((1,), (1,)), ((), ())), preferred_element_type=jnp.float32
        )

    acc[...] = jnp.zeros_like(acc)

    def own_group(group, _):
        start = group * GROUP
        acc[...] += binned(own, start, start, GROUP)
        return 0

    lax.fori_loop(0, BLOCKS // GROUP, own_group, 0)

    for copy in x_copies:
        copy.wait_recv()
    gather(2 * CAP_X, 2, CAP_Z, x_in, z_send)
    z_copies = exchange("gz", 2, z_send, z_in, CAP_Z)
    acc[...] += binned(x_in, 0, BLOCKS, 2 * CAP_X)
    for copy in z_copies:
        copy.wait_recv()
    acc[...] += binned(z_in, 0, BLOCKS + 2 * CAP_X, 2 * CAP_Z)

    y_send[0] = acc[48:72] + acc[72:96]
    y_send[1] = acc[96:120] + acc[120:144]
    y_copies = exchange("gy", 4, y_send, y_in, 1)
    stay = acc[0:24] + acc[24:48]
    for copy in y_copies:
        copy.wait_recv()
    result = stay + y_in[0] + y_in[1]
    out_ref[...] = result[:FIELDS]
    for copy in x_copies + z_copies + y_copies:
        copy.wait_send()


def solution(mesh):
    sizes = dict(mesh.shape)

    def per_device(particle_fields, step_length, live_mask, dest_cell, block_counts, block_lists):
        anywhere = pl.BlockSpec(memory_space=pl.ANY)
        return pl.pallas_call(
            functools.partial(kernel, sizes),
            out_shape=jax.ShapeDtypeStruct((FIELDS, CELLS), jnp.float32),
            in_specs=[anywhere] * 6,
            out_specs=pl.BlockSpec(memory_space=pltpu.VMEM),
            scratch_shapes=[
                pltpu.VMEM((FIELDS, BLOCKS * 128), jnp.float32),
                pltpu.VMEM((BLOCKS, 128), jnp.float32),
                pltpu.VMEM((BLOCKS, 128), jnp.int32),
                pltpu.VMEM((BLOCKS, 128), jnp.int32),
                pltpu.SMEM((1, 6), jnp.int32),
                pltpu.SMEM((1, LIST_LEN), jnp.int32),
                pltpu.VMEM((1, LIST_LEN), jnp.int32),
                pltpu.VMEM((BLOCKS, ROWS, 128), jnp.float32),
                pltpu.VMEM((2 * CAP_X, ROWS, 128), jnp.float32),
                pltpu.VMEM((2 * CAP_X, ROWS, 128), jnp.float32),
                pltpu.VMEM((2 * CAP_Z, ROWS, 128), jnp.float32),
                pltpu.VMEM((2 * CAP_Z, ROWS, 128), jnp.float32),
                pltpu.VMEM((2, ROWS, CELLS), jnp.float32),
                pltpu.VMEM((2, ROWS, CELLS), jnp.float32),
                pltpu.VMEM((3, BLOCKS + 2 * CAP_X + 2 * CAP_Z, 128), jnp.float32),
                pltpu.VMEM((144, CELLS), jnp.float32),
                pltpu.SemaphoreType.DMA((7,)),
                pltpu.SemaphoreType.DMA((6,)),
                pltpu.SemaphoreType.DMA((6,)),
            ],
            compiler_params=pltpu.CompilerParams(collective_id=0, has_side_effects=True),
        )(
            particle_fields,
            step_length.reshape(BLOCKS, 128),
            live_mask.reshape(BLOCKS, 128),
            dest_cell.reshape(BLOCKS, 128),
            block_counts,
            block_lists,
        )

    placed = (P(None, AXES), P(AXES), P(AXES), P(AXES), P(AXES, None), P(AXES, None))
    return jax.shard_map(
        per_device, mesh=mesh, in_specs=placed, out_specs=P(None, AXES), check_vma=False
    )
```

```python
import functools

import jax
import jax.numpy as jnp
from jax import lax
from jax.experimental import pallas as pl
from jax.experimental.pallas import tpu as pltpu
from jax.sharding import PartitionSpec as P

MESH = pl.DeviceIdType.MESH
FIELDS = 20
BLOCKS = 64
CELLS = 512
CAP_X = 6
CAP_Z = 6
CAP_Y = 12
LIST_LEN = 48
ROWS = 24
GROUP = 8
AXES = ("gx", "gy", "gz")


def kernel(
    sizes,
    fields_hbm,
    step_hbm,
    live_hbm,
    cell_hbm,
    counts_hbm,
    lists_hbm,
    out_ref,
    fields,
    step,
    live,
    cell,
    counts,
    lists,
    lists_vec,
    own,
    x_send,
    far_in,
    near_in,
    z_send,
    z_in,
    z_far,
    note_send,
    note_in,
    y_send,
    y_in,
    mask,
    far_mask,
    acc,
    load_sem,
    send_sem,
    recv_sem,
):
    def beside(axis, shift):
        n = sizes[axis]
        return {axis: lax.rem(lax.axis_index(axis) + shift + n, n)}

    loads = [
        pltpu.make_async_copy(source, target, load_sem.at[k])
        for k, (source, target) in enumerate(
            (
                (lists_hbm, lists),
                (counts_hbm, counts),
                (lists_hbm, lists_vec),
                (step_hbm, step),
                (live_hbm, live),
                (cell_hbm, cell),
                (fields_hbm, fields),
            )
        )
    ]
    for load in loads:
        load.start()

    barrier = pltpu.get_barrier_semaphore()
    for axis in AXES:
        for shift in (-1, 1):
            pl.semaphore_signal(
                barrier, inc=1, device_id=beside(axis, shift), device_id_type=MESH
            )
    odd = lax.rem(lax.axis_index("gx"), 2)
    toward_far = 2 * odd - 1
    far_slot, near_slot = CAP_X * odd, CAP_X * (1 - odd)
    far_id, near_id = BLOCKS + far_slot, BLOCKS + near_slot

    for load in loads:
        load.wait()

    row = lax.broadcasted_iota(jnp.int32, (8, 128), 0)

    def carried(block):
        columns = pl.ds(pl.multiple_of(block * 128, 128), 128)
        one = pl.ds(block, 1)
        weight = jnp.broadcast_to(live[one, :].astype(jnp.float32), (8, 128))
        length = jnp.broadcast_to(step[one, :], (8, 128))
        place = jnp.broadcast_to(cell[one, :].astype(jnp.float32), (8, 128))
        first = fields[0:8, columns]
        moved = first + length * pltpu.roll(first, 5, 0)
        first = jnp.where(row < 3, moved, first)
        tail = jnp.where(row[0:4] == 0, place[0:4], 0.0)
        last = jnp.concatenate([fields[16:20, columns] * weight[0:4], tail], axis=0)
        return first * weight, fields[8:16, columns] * weight, last

    def prepare(block, _):
        for k, part in enumerate(carried(block)):
            own[block, 8 * k : 8 * k + 8, :] = part
        return 0

    lax.fori_loop(0, BLOCKS, prepare, 0, unroll=4)

    def usable(first, count, extent, slot):
        entry = lists[0, first + slot]
        return entry, slot % extent < counts[0, count + slot // extent]

    for slot in range(2 * CAP_X):
        entry, valid = usable(0, 0, CAP_X, slot)
        x_send[slot] = jnp.where(valid, own[jnp.clip(entry, 0, BLOCKS - 1)], 0.0)

    def remote(at, source, target, axis, shift):
        copy = pltpu.make_async_remote_copy(
            src_ref=source,
            dst_ref=target,
            send_sem=send_sem.at[at],
            recv_sem=recv_sem.at[at],
            device_id=beside(axis, shift),
            device_id_type=MESH,
        )
        copy.start()
        return copy

    pl.semaphore_wait(barrier, 6)
    far_copies = [
        remote(k, x_send.at[far_slot + k], far_in.at[k], "gx", toward_far)
        for k in range(CAP_X)
    ]
    near_copy = remote(6, x_send.at[pl.ds(near_slot, CAP_X)], near_in, "gx", -toward_far)

    lane = lax.broadcasted_iota(jnp.int32, (1, LIST_LEN), 1)
    limit = jnp.zeros((1, LIST_LEN), jnp.int32)
    begin = 0
    for column, extent in enumerate((CAP_X, CAP_X, CAP_Z, CAP_Z, CAP_Y, CAP_Y)):
        inside = (lane >= begin) & (lane < begin + extent)
        limit = jnp.where(inside, counts[0, column] + begin, limit)
        begin += extent
    named = jnp.where(lane < limit, lists_vec[...], -1)
    note_send[...] = jnp.full_like(note_send, -1.0)
    note_send[:, 0:LIST_LEN] = jnp.broadcast_to(named.astype(jnp.float32), (8, LIST_LEN))

    note_copies = [
        remote(7, note_send, note_in.at[0], "gz", 1),
        remote(8, note_send, note_in.at[1], "gz", -1),
    ]
    near_copy.wait_recv()
    for slot in range(2 * CAP_Z):
        entry, valid = usable(2 * CAP_X, 2, CAP_Z, slot)
        place = entry - near_id
        valid = valid & ((entry < BLOCKS) | ((place >= 0) & (place < CAP_X)))
        chosen = own[jnp.clip(entry, 0, BLOCKS - 1)]
        other = near_in[jnp.clip(place, 0, CAP_X - 1)]
        z_send[slot] = jnp.where(valid, jnp.where(entry < BLOCKS, chosen, other), 0.0)
    z_copies = [
        remote(9, z_send.at[pl.ds(CAP_Z, CAP_Z)], z_in.at[pl.ds(0, CAP_Z)], "gz", 1),
        remote(10, z_send.at[pl.ds(0, CAP_Z)], z_in.at[pl.ds(CAP_Z, CAP_Z)], "gz", -1),
    ]

    total = BLOCKS + 2 * CAP_X + 2 * CAP_Z
    first_y = LIST_LEN - 2 * CAP_Y
    block_id = lax.broadcasted_iota(jnp.int32, (total, LIST_LEN), 0)
    lower = (lane >= first_y) & (lane < first_y + CAP_Y)
    upper = lane >= first_y + CAP_Y
    for k, part in enumerate((named, jnp.where(lower, named, -1), jnp.where(upper, named, -1))):
        found = jnp.max(jnp.where(block_id == part, 1.0, 0.0), axis=1, keepdims=True)
        if k == 0:
            found = 1.0 - found
        mask[k] = jnp.broadcast_to(found, (total, 128))

    tile = lax.broadcasted_iota(jnp.int32, (CELLS, 128), 0).astype(jnp.float32)

    def binned(blocks):
        hot, values = [], ([], [], [])
        for block, weights in blocks:
            hot.append(jnp.where(tile == block[20:21, :], 1.0, 0.0).astype(jnp.bfloat16))
            high = block.astype(jnp.bfloat16).astype(jnp.float32)
            both = jnp.concatenate([high, block - high], axis=0)
            for c in range(3):
                values[c].append((both * weights[c]).astype(jnp.bfloat16))
        left = jnp.concatenate([jnp.concatenate(v, axis=1) for v in values], axis=0)
        right = jnp.concatenate(hot, axis=1)
        return lax.dot_general(
            left, right, (((1,), (1,)), ((), ())), preferred_element_type=jnp.float32
        )

    def weights_of(at):
        return [mask[c, pl.ds(at, 1), :] for c in range(3)]

    acc[...] = jnp.zeros_like(acc)

    def own_group(group, _):
        start = group * GROUP
        acc[...] += binned([(own[start + k], weights_of(start + k)) for k in range(GROUP)])
        return 0

    lax.fori_loop(0, BLOCKS // GROUP, own_group, 0)
    acc[...] += binned([(near_in[k], weights_of(near_id + k)) for k in range(CAP_X)])

    for copy in note_copies:
        copy.wait_recv()
    spot = lax.broadcasted_iota(jnp.int32, (1, 128), 1)
    first_z = 2 * CAP_X
    kept = spot - first_z
    kept = BLOCKS + 2 * CAP_X + jnp.where(kept < CAP_Z, kept + CAP_Z, kept - CAP_Z)
    at_row = lax.broadcasted_iota(jnp.int32, (LIST_LEN, 128), 0)
    at_lane = lax.broadcasted_iota(jnp.int32, (LIST_LEN, 128), 1)
    tall = jnp.broadcast_to(note_send[0:1, :], (LIST_LEN, 128))
    tall = jnp.sum(jnp.where(at_row == at_lane, tall, 0.0), axis=1, keepdims=True)
    same = jnp.where(tall == kept.astype(jnp.float32), 1.0, 0.0)
    down = jnp.max(same[first_y : first_y + CAP_Y], axis=0, keepdims=True)
    up = jnp.max(same[first_y + CAP_Y :], axis=0, keepdims=True)
    stay = 1.0 - down - up
    for side in range(2):
        begin = first_z + CAP_Z * (1 - side)
        inside = (spot >= begin) & (spot < begin + CAP_Z)
        sent = note_in[side] == (row + far_id).astype(jnp.float32)
        for c, kind in enumerate((stay, down, up)):
            hit = jnp.where(sent & inside, kind, 0.0)
            hit = jnp.max(hit, axis=1, keepdims=True)
            far_mask[side, c] = jnp.broadcast_to(hit, (8, 128))

    relays = []
    for k, copy in enumerate(far_copies):
        copy.wait_recv()
        relays.append(
            (
                remote(11 + 2 * k, far_in.at[k], z_far.at[0, k], "gz", 1),
                remote(12 + 2 * k, far_in.at[k], z_far.at[1, k], "gz", -1),
            )
        )
    acc[...] += binned([(far_in[k], weights_of(far_id + k)) for k in range(CAP_X)])
    for copy in z_copies:
        copy.wait_recv()
    z_id = BLOCKS + 2 * CAP_X
    acc[...] += binned([(z_in[k], weights_of(z_id + k)) for k in range(2 * CAP_Z)])
    for k, pair in enumerate(relays):
        for copy in pair:
            copy.wait_recv()
        acc[...] += binned(
            [
                (z_far[side, k], [far_mask[side, c, k : k + 1, :] for c in range(3)])
                for side in range(2)
            ]
        )

    y_send[0] = acc[48:72] + acc[72:96]
    y_send[1] = acc[96:120] + acc[120:144]
    y_copies = [
        remote(23, y_send.at[1], y_in.at[0], "gy", 1),
        remote(24, y_send.at[0], y_in.at[1], "gy", -1),
    ]
    result = acc[0:24] + acc[24:48]
    for copy in y_copies:
        copy.wait_recv()
    result = result + y_in[0] + y_in[1]
    out_ref[...] = result[:FIELDS]
    sent = far_copies + [near_copy] + note_copies + z_copies + y_copies
    for copy in sent + [copy for pair in relays for copy in pair]:
        copy.wait_send()


def solution(mesh):
    sizes = dict(mesh.shape)

    def per_device(particle_fields, step_length, live_mask, dest_cell, block_counts, block_lists):
        anywhere = pl.BlockSpec(memory_space=pl.ANY)
        return pl.pallas_call(
            functools.partial(kernel, sizes),
            out_shape=pltpu.VMEM((FIELDS, CELLS), jnp.float32),
            in_specs=[anywhere] * 6,
            out_specs=pl.BlockSpec(memory_space=pltpu.VMEM),
            scratch_shapes=[
                pltpu.VMEM((FIELDS, BLOCKS * 128), jnp.float32),
                pltpu.VMEM((BLOCKS, 128), jnp.float32),
                pltpu.VMEM((BLOCKS, 128), jnp.int32),
                pltpu.VMEM((BLOCKS, 128), jnp.int32),
                pltpu.SMEM((1, 6), jnp.int32),
                pltpu.SMEM((1, LIST_LEN), jnp.int32),
                pltpu.VMEM((1, LIST_LEN), jnp.int32),
                pltpu.VMEM((BLOCKS, ROWS, 128), jnp.float32),
                pltpu.VMEM((2 * CAP_X, ROWS, 128), jnp.float32),
                pltpu.VMEM((CAP_X, ROWS, 128), jnp.float32),
                pltpu.VMEM((CAP_X, ROWS, 128), jnp.float32),
                pltpu.VMEM((2 * CAP_Z, ROWS, 128), jnp.float32),
                pltpu.VMEM((2 * CAP_Z, ROWS, 128), jnp.float32),
                pltpu.VMEM((2, CAP_X, ROWS, 128), jnp.float32),
                pltpu.VMEM((8, 128), jnp.float32),
                pltpu.VMEM((2, 8, 128), jnp.float32),
                pltpu.VMEM((2, ROWS, CELLS), jnp.float32),
                pltpu.VMEM((2, ROWS, CELLS), jnp.float32),
                pltpu.VMEM((3, BLOCKS + 2 * CAP_X + 2 * CAP_Z, 128), jnp.float32),
                pltpu.VMEM((2, 3, 8, 128), jnp.float32),
                pltpu.VMEM((144, CELLS), jnp.float32),
                pltpu.SemaphoreType.DMA((7,)),
                pltpu.SemaphoreType.DMA((25,)),
                pltpu.SemaphoreType.DMA((25,)),
            ],
            compiler_params=pltpu.CompilerParams(collective_id=0, has_side_effects=True),
        )(
            particle_fields,
            step_length.reshape(BLOCKS, 128),
            live_mask.reshape(BLOCKS, 128),
            dest_cell.reshape(BLOCKS, 128),
            block_counts,
            block_lists,
        )

    placed = (P(None, AXES), P(AXES), P(AXES), P(AXES), P(AXES, None), P(AXES, None))
    return jax.shard_map(
        per_device, mesh=mesh, in_specs=placed, out_specs=P(None, AXES), check_vma=False
    )
```

```python
import functools

import jax
import jax.numpy as jnp
from jax import lax
from jax.experimental import pallas as pl
from jax.experimental.pallas import tpu as pltpu
from jax.sharding import PartitionSpec as P

MESH = pl.DeviceIdType.MESH
FIELDS = 20
BLOCKS = 64
CELLS = 512
CAP_X = 6
CAP_Z = 6
CAP_Y = 12
LIST_LEN = 48
ROWS = 24
GROUP = 8
PARTS = ((0, 2), (2, 2), (4, 2))
AXES = ("gx", "gy", "gz")


def kernel(
    sizes,
    fields_hbm,
    step_hbm,
    live_hbm,
    cell_hbm,
    counts_hbm,
    lists_hbm,
    out_ref,
    fields,
    step,
    live,
    cell,
    counts,
    lists,
    lists_vec,
    own,
    x_send,
    far_in,
    near_in,
    z_send,
    z_in,
    z_far,
    note_send,
    note_in,
    y_send,
    y_in,
    mask,
    far_mask,
    acc,
    load_sem,
    send_sem,
    recv_sem,
    ready,
):
    def beside(axis, shift):
        n = sizes[axis]
        return {axis: lax.rem(lax.axis_index(axis) + shift + n, n)}

    loads = [
        pltpu.make_async_copy(source, target, load_sem.at[k])
        for k, (source, target) in enumerate(
            (
                (lists_hbm, lists),
                (counts_hbm, counts),
                (lists_hbm, lists_vec),
                (step_hbm, step),
                (live_hbm, live),
                (cell_hbm, cell),
                (fields_hbm, fields),
            )
        )
    ]
    for load in loads:
        load.start()

    gx = lax.axis_index("gx")
    odd = lax.rem(gx, 2)
    toward_far = 2 * odd - 1
    early = (gx == 0) | ((odd == 1) & (gx != sizes["gx"] - 1))
    barrier = pltpu.get_barrier_semaphore()

    def greet(axis, shift):
        pl.semaphore_signal(barrier, inc=1, device_id=beside(axis, shift), device_id_type=MESH)

    for axis, shift in (("gz", -1), ("gz", 1), ("gy", -1), ("gy", 1), ("gx", -toward_far)):
        greet(axis, shift)

    @pl.when(early)
    def _():
        greet("gx", toward_far)

    far_slot, near_slot = CAP_X * odd, CAP_X * (1 - odd)
    far_id, near_id = BLOCKS + far_slot, BLOCKS + near_slot

    for load in loads:
        load.wait()

    row = lax.broadcasted_iota(jnp.int32, (8, 128), 0)

    def carried(block):
        columns = pl.ds(pl.multiple_of(block * 128, 128), 128)
        one = pl.ds(block, 1)
        weight = jnp.broadcast_to(live[one, :].astype(jnp.float32), (8, 128))
        length = jnp.broadcast_to(step[one, :], (8, 128))
        place = jnp.broadcast_to(cell[one, :].astype(jnp.float32), (8, 128))
        first = fields[0:8, columns]
        moved = first + length * pltpu.roll(first, 5, 0)
        first = jnp.where(row < 3, moved, first)
        tail = jnp.where(row[0:4] == 0, place[0:4], 0.0)
        last = jnp.concatenate([fields[16:20, columns] * weight[0:4], tail], axis=0)
        return first * weight, fields[8:16, columns] * weight, last

    def prepare(block, _):
        for k, part in enumerate(carried(block)):
            own[block, 8 * k : 8 * k + 8, :] = part
        return 0

    lax.fori_loop(0, BLOCKS, prepare, 0, unroll=4)

    def usable(first, count, extent, slot):
        entry = lists[0, first + slot]
        return entry, slot % extent < counts[0, count + slot // extent]

    for slot in range(2 * CAP_X):
        entry, valid = usable(0, 0, CAP_X, slot)
        x_send[slot] = jnp.where(valid, own[jnp.clip(entry, 0, BLOCKS - 1)], 0.0)

    def describe(at, source, target, axis, shift):
        return pltpu.make_async_remote_copy(
            src_ref=source,
            dst_ref=target,
            send_sem=send_sem.at[at],
            recv_sem=recv_sem.at[at],
            device_id=beside(axis, shift),
            device_id_type=MESH,
        )

    def remote(*where):
        copy = describe(*where)
        copy.start()
        return copy

    pl.semaphore_wait(barrier, jnp.where(early, 5, 6))
    far_copies = []
    for k, (at, size) in enumerate(PARTS):
        source = x_send.at[pl.ds(far_slot + at, size)]
        far_copies.append(describe(k, source, far_in.at[pl.ds(at, size)], "gx", toward_far))

    @pl.when(jnp.logical_not(early))
    def _():
        pl.semaphore_signal(
            ready, inc=1, device_id=beside("gx", toward_far), device_id_type=MESH
        )
        for copy in far_copies:
            copy.start()

    near_copy = remote(6, x_send.at[pl.ds(near_slot, CAP_X)], near_in, "gx", -toward_far)

    lane = lax.broadcasted_iota(jnp.int32, (1, LIST_LEN), 1)
    limit = jnp.zeros((1, LIST_LEN), jnp.int32)
    begin = 0
    for column, extent in enumerate((CAP_X, CAP_X, CAP_Z, CAP_Z, CAP_Y, CAP_Y)):
        inside = (lane >= begin) & (lane < begin + extent)
        limit = jnp.where(inside, counts[0, column] + begin, limit)
        begin += extent
    named = jnp.where(lane < limit, lists_vec[...], -1)
    note_send[...] = jnp.full_like(note_send, -1.0)
    note_send[:, 0:LIST_LEN] = jnp.broadcast_to(named.astype(jnp.float32), (8, LIST_LEN))

    note_copies = [
        remote(7, note_send, note_in.at[0], "gz", 1),
        remote(8, note_send, note_in.at[1], "gz", -1),
    ]
    near_copy.wait_recv()
    for slot in range(2 * CAP_Z):
        entry, valid = usable(2 * CAP_X, 2, CAP_Z, slot)
        place = entry - near_id
        valid = valid & ((entry < BLOCKS) | ((place >= 0) & (place < CAP_X)))
        chosen = own[jnp.clip(entry, 0, BLOCKS - 1)]
        other = near_in[jnp.clip(place, 0, CAP_X - 1)]
        z_send[slot] = jnp.where(valid, jnp.where(entry < BLOCKS, chosen, other), 0.0)
    z_copies = [
        remote(9, z_send.at[pl.ds(CAP_Z, CAP_Z)], z_in.at[pl.ds(0, CAP_Z)], "gz", 1),
        remote(10, z_send.at[pl.ds(0, CAP_Z)], z_in.at[pl.ds(CAP_Z, CAP_Z)], "gz", -1),
    ]

    total = BLOCKS + 2 * CAP_X + 2 * CAP_Z
    first_y = LIST_LEN - 2 * CAP_Y
    block_id = lax.broadcasted_iota(jnp.int32, (total, LIST_LEN), 0)
    lower = (lane >= first_y) & (lane < first_y + CAP_Y)
    upper = lane >= first_y + CAP_Y
    for k, part in enumerate((named, jnp.where(lower, named, -1), jnp.where(upper, named, -1))):
        found = jnp.max(jnp.where(block_id == part, 1.0, 0.0), axis=1, keepdims=True)
        if k == 0:
            found = 1.0 - found
        mask[k] = jnp.broadcast_to(found, (total, 128))

    tile = lax.broadcasted_iota(jnp.int32, (CELLS, 128), 0).astype(jnp.float32)

    def binned(blocks):
        hot, values = [], ([], [], [])
        for block, weights in blocks:
            hot.append(jnp.where(tile == block[20:21, :], 1.0, 0.0).astype(jnp.bfloat16))
            high = block.astype(jnp.bfloat16).astype(jnp.float32)
            both = jnp.concatenate([high, block - high], axis=0)
            for c in range(3):
                values[c].append((both * weights[c]).astype(jnp.bfloat16))
        left = jnp.concatenate([jnp.concatenate(v, axis=1) for v in values], axis=0)
        right = jnp.concatenate(hot, axis=1)
        return lax.dot_general(
            left, right, (((1,), (1,)), ((), ())), preferred_element_type=jnp.float32
        )

    def weights_of(at):
        return [mask[c, pl.ds(at, 1), :] for c in range(3)]

    acc[...] = jnp.zeros_like(acc)

    def own_group(group, _):
        start = group * GROUP
        acc[...] += binned([(own[start + k], weights_of(start + k)) for k in range(GROUP)])
        return 0

    lax.fori_loop(0, BLOCKS // GROUP, own_group, 0)
    acc[...] += binned([(near_in[k], weights_of(near_id + k)) for k in range(CAP_X)])

    for copy in note_copies:
        copy.wait_recv()
    spot = lax.broadcasted_iota(jnp.int32, (1, 128), 1)
    first_z = 2 * CAP_X
    kept = spot - first_z
    kept = BLOCKS + 2 * CAP_X + jnp.where(kept < CAP_Z, kept + CAP_Z, kept - CAP_Z)
    at_row = lax.broadcasted_iota(jnp.int32, (LIST_LEN, 128), 0)
    at_lane = lax.broadcasted_iota(jnp.int32, (LIST_LEN, 128), 1)
    tall = jnp.broadcast_to(note_send[0:1, :], (LIST_LEN, 128))
    tall = jnp.sum(jnp.where(at_row == at_lane, tall, 0.0), axis=1, keepdims=True)
    same = jnp.where(tall == kept.astype(jnp.float32), 1.0, 0.0)
    down = jnp.max(same[first_y : first_y + CAP_Y], axis=0, keepdims=True)
    up = jnp.max(same[first_y + CAP_Y :], axis=0, keepdims=True)
    stay = 1.0 - down - up
    for side in range(2):
        begin = first_z + CAP_Z * (1 - side)
        inside = (spot >= begin) & (spot < begin + CAP_Z)
        sent = note_in[side] == (row + far_id).astype(jnp.float32)
        for c, kind in enumerate((stay, down, up)):
            hit = jnp.where(sent & inside, kind, 0.0)
            hit = jnp.max(hit, axis=1, keepdims=True)
            far_mask[side, c] = jnp.broadcast_to(hit, (8, 128))

    for copy in z_copies:
        copy.wait_recv()
    z_id = BLOCKS + 2 * CAP_X
    acc[...] += binned([(z_in[k], weights_of(z_id + k)) for k in range(2 * CAP_Z)])

    @pl.when(early)
    def _():
        pl.semaphore_wait(ready, 1)
        for copy in far_copies:
            copy.start()

    relays = []
    for k, copy in enumerate(far_copies):
        copy.wait_recv()
        part = pl.ds(*PARTS[k])
        relays.append(
            (
                remote(11 + 2 * k, far_in.at[part], z_far.at[0, part], "gz", 1),
                remote(12 + 2 * k, far_in.at[part], z_far.at[1, part], "gz", -1),
            )
        )
    acc[...] += binned([(far_in[k], weights_of(far_id + k)) for k in range(CAP_X)])
    for (at, size), pair in zip(PARTS, relays, strict=True):
        for copy in pair:
            copy.wait_recv()
        acc[...] += binned(
            [
                (z_far[side, k], [far_mask[side, c, k : k + 1, :] for c in range(3)])
                for k in range(at, at + size)
                for side in range(2)
            ]
        )

    y_send[0] = acc[48:72] + acc[72:96]
    y_send[1] = acc[96:120] + acc[120:144]
    y_copies = [
        remote(23, y_send.at[1], y_in.at[0], "gy", 1),
        remote(24, y_send.at[0], y_in.at[1], "gy", -1),
    ]
    result = acc[0:24] + acc[24:48]
    for copy in y_copies:
        copy.wait_recv()
    result = result + y_in[0] + y_in[1]
    out_ref[...] = result[:FIELDS]
    sent = far_copies + [near_copy] + note_copies + z_copies + y_copies
    for copy in sent + [copy for pair in relays for copy in pair]:
        copy.wait_send()


def solution(mesh):
    sizes = dict(mesh.shape)

    def per_device(particle_fields, step_length, live_mask, dest_cell, block_counts, block_lists):
        anywhere = pl.BlockSpec(memory_space=pl.ANY)
        return pl.pallas_call(
            functools.partial(kernel, sizes),
            out_shape=pltpu.VMEM((FIELDS, CELLS), jnp.float32),
            in_specs=[anywhere] * 6,
            out_specs=pl.BlockSpec(memory_space=pltpu.VMEM),
            scratch_shapes=[
                pltpu.VMEM((FIELDS, BLOCKS * 128), jnp.float32),
                pltpu.VMEM((BLOCKS, 128), jnp.float32),
                pltpu.VMEM((BLOCKS, 128), jnp.int32),
                pltpu.VMEM((BLOCKS, 128), jnp.int32),
                pltpu.SMEM((1, 6), jnp.int32),
                pltpu.SMEM((1, LIST_LEN), jnp.int32),
                pltpu.VMEM((1, LIST_LEN), jnp.int32),
                pltpu.VMEM((BLOCKS, ROWS, 128), jnp.float32),
                pltpu.VMEM((2 * CAP_X, ROWS, 128), jnp.float32),
                pltpu.VMEM((CAP_X, ROWS, 128), jnp.float32),
                pltpu.VMEM((CAP_X, ROWS, 128), jnp.float32),
                pltpu.VMEM((2 * CAP_Z, ROWS, 128), jnp.float32),
                pltpu.VMEM((2 * CAP_Z, ROWS, 128), jnp.float32),
                pltpu.VMEM((2, CAP_X, ROWS, 128), jnp.float32),
                pltpu.VMEM((8, 128), jnp.float32),
                pltpu.VMEM((2, 8, 128), jnp.float32),
                pltpu.VMEM((2, ROWS, CELLS), jnp.float32),
                pltpu.VMEM((2, ROWS, CELLS), jnp.float32),
                pltpu.VMEM((3, BLOCKS + 2 * CAP_X + 2 * CAP_Z, 128), jnp.float32),
                pltpu.VMEM((2, 3, 8, 128), jnp.float32),
                pltpu.VMEM((144, CELLS), jnp.float32),
                pltpu.SemaphoreType.DMA((7,)),
                pltpu.SemaphoreType.DMA((25,)),
                pltpu.SemaphoreType.DMA((25,)),
                pltpu.SemaphoreType.REGULAR,
            ],
            compiler_params=pltpu.CompilerParams(collective_id=0, has_side_effects=True),
        )(
            particle_fields,
            step_length.reshape(BLOCKS, 128),
            live_mask.reshape(BLOCKS, 128),
            dest_cell.reshape(BLOCKS, 128),
            block_counts,
            block_lists,
        )

    placed = (P(None, AXES), P(AXES), P(AXES), P(AXES), P(AXES, None), P(AXES, None))
    return jax.shard_map(
        per_device, mesh=mesh, in_specs=placed, out_specs=P(None, AXES), check_vma=False
    )
```

```python
import functools

import jax
import jax.numpy as jnp
from jax import lax
from jax.experimental import pallas as pl
from jax.experimental.pallas import tpu as pltpu
from jax.sharding import PartitionSpec as P

MESH = pl.DeviceIdType.MESH
FIELDS = 20
BLOCKS = 64
CELLS = 512
CAP_X = 6
CAP_Z = 6
CAP_Y = 12
LIST_LEN = 48
ROWS = 24
GROUP = 8
PARTS = ((0, 2), (2, 2), (4, 2))
SENDS = ((1, 1), (1, -1), (-1, 1), (-1, -1), (0, 1), (0, -1), (1, 0), (-1, 0))
CLASS = {0: 0, -1: 1, 1: 2}
AXES = ("gx", "gy", "gz")


def kernel(
    sizes,
    fields_hbm,
    step_hbm,
    live_hbm,
    cell_hbm,
    counts_hbm,
    lists_hbm,
    out_ref,
    fields,
    step,
    live,
    cell,
    counts,
    lists,
    lists_vec,
    own,
    x_send,
    far_in,
    near_in,
    list_row,
    note_send,
    note_in,
    sum_send,
    sum_in,
    mask,
    acc,
    load_sem,
    send_sem,
    recv_sem,
    ready,
):
    def beside(**shifts):
        return {
            axis: lax.rem(lax.axis_index(axis) + shift + sizes[axis], sizes[axis])
            for axis, shift in shifts.items()
        }

    loads = [
        pltpu.make_async_copy(source, target, load_sem.at[k])
        for k, (source, target) in enumerate(
            (
                (lists_hbm, lists),
                (counts_hbm, counts),
                (lists_hbm, lists_vec),
                (step_hbm, step),
                (live_hbm, live),
                (cell_hbm, cell),
                (fields_hbm, fields),
            )
        )
    ]
    for load in loads:
        load.start()

    gx = lax.axis_index("gx")
    odd = lax.rem(gx, 2)
    toward_far = 2 * odd - 1
    early = (gx == 0) | ((odd == 1) & (gx != sizes["gx"] - 1))
    barrier = pltpu.get_barrier_semaphore()

    def greet(where):
        pl.semaphore_signal(barrier, inc=1, device_id=where, device_id_type=MESH)

    greet(beside(gx=-toward_far))
    for dz, dy in SENDS:
        greet(beside(gz=dz, gy=dy))

    @pl.when(early)
    def _():
        greet(beside(gx=toward_far))

    far_slot, near_slot = CAP_X * odd, CAP_X * (1 - odd)
    far_id, near_id = BLOCKS + far_slot, BLOCKS + near_slot

    for load in loads:
        load.wait()

    row = lax.broadcasted_iota(jnp.int32, (8, 128), 0)

    def prepare(block, _):
        columns = pl.ds(pl.multiple_of(block * 128, 128), 128)
        one = pl.ds(block, 1)
        weight = jnp.broadcast_to(live[one, :].astype(jnp.float32), (8, 128))
        length = jnp.broadcast_to(step[one, :], (8, 128))
        place = jnp.broadcast_to(cell[one, :].astype(jnp.float32), (8, 128))
        first = fields[0:8, columns]
        moved = first + length * pltpu.roll(first, 5, 0)
        first = jnp.where(row < 3, moved, first)
        tail = jnp.where(row[0:4] == 0, place[0:4], 0.0)
        last = jnp.concatenate([fields[16:20, columns] * weight[0:4], tail], axis=0)
        own[block, 0:8, :] = first * weight
        own[block, 8:16, :] = fields[8:16, columns] * weight
        own[block, 16:24, :] = last
        return 0

    lax.fori_loop(0, BLOCKS, prepare, 0, unroll=8)

    for slot in range(2 * CAP_X):
        valid = slot % CAP_X < counts[0, slot // CAP_X]
        entry = jnp.clip(lists[0, slot], 0, BLOCKS - 1)
        x_send[slot] = jnp.where(valid, own[entry], 0.0)

    def describe(at, source, target, where):
        return pltpu.make_async_remote_copy(
            src_ref=source,
            dst_ref=target,
            send_sem=send_sem.at[at],
            recv_sem=recv_sem.at[at],
            device_id=where,
            device_id_type=MESH,
        )

    def remote(*what):
        copy = describe(*what)
        copy.start()
        return copy

    pl.semaphore_wait(barrier, jnp.where(early, len(SENDS) + 1, len(SENDS) + 2))
    far_copies = []
    for k, (at, size) in enumerate(PARTS):
        source = x_send.at[pl.ds(far_slot + at, size)]
        target = far_in.at[pl.ds(at, size)]
        far_copies.append(describe(k, source, target, beside(gx=toward_far)))

    @pl.when(jnp.logical_not(early))
    def _():
        pl.semaphore_signal(
            ready, inc=1, device_id=beside(gx=toward_far), device_id_type=MESH
        )
        for copy in far_copies:
            copy.start()

    at = len(PARTS)
    near_copy = remote(
        at, x_send.at[pl.ds(near_slot, CAP_X)], near_in, beside(gx=-toward_far)
    )

    lane = lax.broadcasted_iota(jnp.int32, (1, LIST_LEN), 1)
    limit = jnp.zeros((1, LIST_LEN), jnp.int32)
    begin = 0
    for column, extent in enumerate((CAP_X, CAP_X, CAP_Z, CAP_Z, CAP_Y, CAP_Y)):
        inside = (lane >= begin) & (lane < begin + extent)
        limit = jnp.where(inside, counts[0, column] + begin, limit)
        begin += extent
    named = jnp.where(lane < limit, lists_vec[...], -1).astype(jnp.float32)
    list_row[...] = jnp.full_like(list_row, -1.0)
    list_row[:, 0:LIST_LEN] = jnp.broadcast_to(named, (8, LIST_LEN))
    named = list_row[0:1, :]
    spot = lax.broadcasted_iota(jnp.int32, (1, 128), 1)
    first_z, first_y = 2 * CAP_X, 2 * CAP_X + 2 * CAP_Z
    offset = spot - first_z
    kept = BLOCKS + 2 * CAP_X + jnp.where(offset < CAP_Z, offset + CAP_Z, offset - CAP_Z)
    at_row = lax.broadcasted_iota(jnp.int32, (LIST_LEN, 128), 0)
    at_lane = lax.broadcasted_iota(jnp.int32, (LIST_LEN, 128), 1)
    tall = jnp.broadcast_to(named, (LIST_LEN, 128))
    tall = jnp.sum(jnp.where(at_row == at_lane, tall, 0.0), axis=1, keepdims=True)
    same = jnp.where(tall == kept.astype(jnp.float32), 1.0, 0.0)
    down = jnp.max(same[first_y : first_y + CAP_Y], axis=0, keepdims=True)
    up = jnp.max(same[first_y + CAP_Y :], axis=0, keepdims=True)
    note_send[...] = jnp.where(row == 0, 1.0 - down - up, jnp.where(row == 1, down, up))
    note_copies = [
        remote(at + 1, note_send, note_in.at[0], beside(gz=1)),
        remote(at + 2, note_send, note_in.at[1], beside(gz=-1)),
    ]
    at += 3

    total = mask.shape[1]
    block_id = lax.broadcasted_iota(jnp.int32, (total, 128), 0).astype(jnp.float32)
    hit = jnp.where(block_id == named, 1.0, 0.0)

    def between(start, extent):
        return jnp.where((spot >= start) & (spot < start + extent), 1.0, 0.0)

    def select(c, lanes):
        found = jnp.max(hit * lanes, axis=1, keepdims=True)
        if c == 0:
            found = 1.0 - found
        mask[c] = jnp.broadcast_to(found, (total, 128))

    select(0, jnp.ones((1, 128), jnp.float32))
    select(1, between(first_y, CAP_Y))
    select(2, between(first_y + CAP_Y, CAP_Y))
    acc[...] = jnp.zeros_like(acc)
    for copy in note_copies:
        copy.wait_recv()
    for side in range(2):
        part = between(first_z + CAP_Z * side, CAP_Z)
        for kind in range(3):
            select(3 + 3 * side + kind, note_in[side, kind : kind + 1, :] * part)

    tile = lax.broadcasted_iota(jnp.int32, (CELLS, 128), 0).astype(jnp.float32)

    def binned(source, start, first_id, count):
        hot, values = [], [[] for _ in range(9)]
        for k in range(count):
            block = source[start + k]
            hot.append(jnp.where(tile == block[20:21, :], 1.0, 0.0).astype(jnp.bfloat16))
            high = block.astype(jnp.bfloat16).astype(jnp.float32)
            both = jnp.concatenate([high, block - high], axis=0)
            for c in range(9):
                weight = mask[c, pl.ds(first_id + k, 1), :]
                values[c].append((both * weight).astype(jnp.bfloat16))
        left = jnp.concatenate([jnp.concatenate(v, axis=1) for v in values], axis=0)
        right = jnp.concatenate(hot, axis=1)
        return lax.dot_general(
            left, right, (((1,), (1,)), ((), ())), preferred_element_type=jnp.float32
        )

    def own_group(group, _):
        start = group * GROUP
        acc[...] += binned(own, start, start, GROUP)
        return 0

    lax.fori_loop(0, BLOCKS // GROUP, own_group, 0)
    near_copy.wait_recv()
    acc[...] += binned(near_in, 0, near_id, CAP_X)

    @pl.when(early)
    def _():
        pl.semaphore_wait(ready, 1)
        for copy in far_copies:
            copy.start()

    for (start, size), copy in zip(PARTS, far_copies, strict=True):
        copy.wait_recv()
        acc[...] += binned(far_in, start, far_id + start, size)

    def packed(dz, dy):
        first = 144 * CLASS[dz] + 48 * CLASS[dy]
        sums = acc[first : first + 24] + acc[first + 24 : first + 48]
        tiles = [sums[8 * r : 8 * r + 8, 128 * k : 128 * k + 128] for r in (0, 1) for k in range(4)]
        for k in (0, 256):
            pair = [sums[16:20, k : k + 128], sums[16:20, k + 128 : k + 256]]
            tiles.append(jnp.concatenate(pair, axis=0))
        return tiles

    sum_copies = []
    for m, (dz, dy) in enumerate(SENDS):
        for k, part in enumerate(packed(dz, dy)):
            sum_send[m, k] = part
        sum_copies.append(
            remote(at + m, sum_send.at[m], sum_in.at[m], beside(gz=dz, gy=dy))
        )
    result = packed(0, 0)
    for m, copy in enumerate(sum_copies):
        copy.wait_recv()
        result = [part + sum_in[m, k] for k, part in enumerate(result)]
    for k in range(4):
        columns = slice(128 * k, 128 * k + 128)
        out_ref[0:8, columns] = result[k]
        out_ref[8:16, columns] = result[4 + k]
        half = 4 * (k % 2)
        out_ref[16:20, columns] = result[8 + k // 2][half : half + 4]
    for copy in far_copies + [near_copy] + note_copies + sum_copies:
        copy.wait_send()


def solution(mesh):
    sizes = dict(mesh.shape)

    def per_device(particle_fields, step_length, live_mask, dest_cell, block_counts, block_lists):
        anywhere = pl.BlockSpec(memory_space=pl.ANY)
        copies = len(PARTS) + 3 + len(SENDS)
        return pl.pallas_call(
            functools.partial(kernel, sizes),
            out_shape=pltpu.VMEM((FIELDS, CELLS), jnp.float32),
            in_specs=[anywhere] * 6,
            out_specs=pl.BlockSpec(memory_space=pltpu.VMEM),
            scratch_shapes=[
                pltpu.VMEM((FIELDS, BLOCKS * 128), jnp.float32),
                pltpu.VMEM((BLOCKS, 128), jnp.float32),
                pltpu.VMEM((BLOCKS, 128), jnp.int32),
                pltpu.VMEM((BLOCKS, 128), jnp.int32),
                pltpu.SMEM((1, 6), jnp.int32),
                pltpu.SMEM((1, LIST_LEN), jnp.int32),
                pltpu.VMEM((1, LIST_LEN), jnp.int32),
                pltpu.VMEM((BLOCKS, ROWS, 128), jnp.float32),
                pltpu.VMEM((2 * CAP_X, ROWS, 128), jnp.float32),
                pltpu.VMEM((CAP_X, ROWS, 128), jnp.float32),
                pltpu.VMEM((CAP_X, ROWS, 128), jnp.float32),
                pltpu.VMEM((8, 128), jnp.float32),
                pltpu.VMEM((8, 128), jnp.float32),
                pltpu.VMEM((2, 8, 128), jnp.float32),
                pltpu.VMEM((len(SENDS), 10, 8, 128), jnp.float32),
                pltpu.VMEM((len(SENDS), 10, 8, 128), jnp.float32),
                pltpu.VMEM((9, BLOCKS + 16, 128), jnp.float32),
                pltpu.VMEM((9 * 2 * ROWS, CELLS), jnp.float32),
                pltpu.SemaphoreType.DMA((7,)),
                pltpu.SemaphoreType.DMA((copies,)),
                pltpu.SemaphoreType.DMA((copies,)),
                pltpu.SemaphoreType.REGULAR,
            ],
            compiler_params=pltpu.CompilerParams(collective_id=0, has_side_effects=True),
        )(
            particle_fields,
            step_length.reshape(BLOCKS, 128),
            live_mask.reshape(BLOCKS, 128),
            dest_cell.reshape(BLOCKS, 128),
            block_counts,
            block_lists,
        )

    placed = (P(None, AXES), P(AXES), P(AXES), P(AXES), P(AXES, None), P(AXES, None))
    return jax.shard_map(
        per_device, mesh=mesh, in_specs=placed, out_specs=P(None, AXES), check_vma=False
    )
```

```python
import functools

import jax
import jax.numpy as jnp
from jax import lax
from jax.experimental import pallas as pl
from jax.experimental.pallas import tpu as pltpu
from jax.sharding import PartitionSpec as P

MESH = pl.DeviceIdType.MESH
FIELDS = 20
BLOCKS = 64
CELLS = 512
CAP_X = 6
CAP_Z = 6
CAP_Y = 12
LIST_LEN = 48
ROWS = 24
GROUP = 8
PARTS = ((0, 6), (6, 5), (11, 5))
SENDS = ((1, 1), (1, -1), (-1, 1), (-1, -1), (0, 1), (0, -1), (1, 0), (-1, 0))
CLASS = {0: 0, -1: 1, 1: 2}
AXES = ("gx", "gy", "gz")


def kernel(
    sizes,
    fields_hbm,
    step_hbm,
    live_hbm,
    cell_hbm,
    counts_hbm,
    lists_hbm,
    out_ref,
    fields,
    step,
    live,
    cell,
    counts,
    lists,
    lists_vec,
    own,
    far_send,
    near_send,
    far_in,
    near_in,
    list_row,
    note_send,
    note_in,
    sum_send,
    sum_in,
    mask,
    far_mask,
    slot_mask,
    acc,
    load_sem,
    send_sem,
    recv_sem,
    ready,
):
    def beside(**shifts):
        return {
            axis: lax.rem(lax.axis_index(axis) + shift + sizes[axis], sizes[axis])
            for axis, shift in shifts.items()
        }

    loads = [
        pltpu.make_async_copy(source, target, load_sem.at[k])
        for k, (source, target) in enumerate(
            (
                (lists_hbm, lists),
                (counts_hbm, counts),
                (lists_hbm, lists_vec),
                (step_hbm, step),
                (live_hbm, live),
                (cell_hbm, cell),
                (fields_hbm, fields),
            )
        )
    ]
    for load in loads:
        load.start()

    gx = lax.axis_index("gx")
    odd = lax.rem(gx, 2)
    toward_far = 2 * odd - 1
    early = (gx == 0) | ((odd == 1) & (gx != sizes["gx"] - 1))
    barrier = pltpu.get_barrier_semaphore()

    def greet(where):
        pl.semaphore_signal(barrier, inc=1, device_id=where, device_id_type=MESH)

    greet(beside(gx=-toward_far))
    for dz, dy in SENDS:
        greet(beside(gz=dz, gy=dy))

    @pl.when(early)
    def _():
        greet(beside(gx=toward_far))

    far_slot, near_slot = CAP_X * odd, CAP_X * (1 - odd)
    far_id, near_id = BLOCKS + far_slot, BLOCKS + near_slot

    for load in loads:
        load.wait()

    row = lax.broadcasted_iota(jnp.int32, (8, 128), 0)

    def prepare(block, _):
        columns = pl.ds(pl.multiple_of(block * 128, 128), 128)
        one = pl.ds(block, 1)
        weight = jnp.broadcast_to(live[one, :].astype(jnp.float32), (8, 128))
        length = jnp.broadcast_to(step[one, :], (8, 128))
        place = jnp.broadcast_to(cell[one, :].astype(jnp.float32), (8, 128))
        first = fields[0:8, columns]
        moved = first + length * pltpu.roll(first, 5, 0)
        first = jnp.where(row < 3, moved, first)
        tail = jnp.where(row[0:4] == 0, place[0:4], 0.0)
        last = jnp.concatenate([fields[16:20, columns] * weight[0:4], tail], axis=0)
        own[block, 0:8, :] = first * weight
        own[block, 8:16, :] = fields[8:16, columns] * weight
        own[block, 16:24, :] = last
        return 0

    lax.fori_loop(0, BLOCKS, prepare, 0, unroll=8)

    tops, cells = [], jnp.zeros((8, 128), jnp.float32)
    for k in range(CAP_X):
        entry = jnp.clip(lists[0, far_slot + k], 0, BLOCKS - 1)
        block = jnp.where(k < counts[0, odd], own[entry], 0.0)
        tops.append(block[16:24])
        cells = jnp.where(row == k, block[20:21], cells)
        at = 1 + 5 * (k // 2) + 2 * (k % 2)
        far_send[at] = block[0:8]
        far_send[at + 1] = block[8:16]
        if k % 2:
            far_send[at + 2] = jnp.where(row < 4, tops[k - 1], pltpu.roll(tops[k], 4, 0))
    far_send[0] = cells
    for k in range(CAP_X):
        entry = jnp.clip(lists[0, near_slot + k], 0, BLOCKS - 1)
        near_send[k] = jnp.where(k < counts[0, 1 - odd], own[entry], 0.0)

    def describe(at, source, target, where):
        return pltpu.make_async_remote_copy(
            src_ref=source,
            dst_ref=target,
            send_sem=send_sem.at[at],
            recv_sem=recv_sem.at[at],
            device_id=where,
            device_id_type=MESH,
        )

    def remote(*what):
        copy = describe(*what)
        copy.start()
        return copy

    pl.semaphore_wait(barrier, jnp.where(early, len(SENDS) + 1, len(SENDS) + 2))
    far_copies = []
    for k, part in enumerate(PARTS):
        source, target = far_send.at[pl.ds(*part)], far_in.at[pl.ds(*part)]
        far_copies.append(describe(k, source, target, beside(gx=toward_far)))

    @pl.when(jnp.logical_not(early))
    def _():
        pl.semaphore_signal(
            ready, inc=1, device_id=beside(gx=toward_far), device_id_type=MESH
        )
        for copy in far_copies:
            copy.start()

    at = len(PARTS)
    near_copy = remote(at, near_send, near_in, beside(gx=-toward_far))

    lane = lax.broadcasted_iota(jnp.int32, (1, LIST_LEN), 1)
    limit = jnp.zeros((1, LIST_LEN), jnp.int32)
    begin = 0
    for column, extent in enumerate((CAP_X, CAP_X, CAP_Z, CAP_Z, CAP_Y, CAP_Y)):
        inside = (lane >= begin) & (lane < begin + extent)
        limit = jnp.where(inside, counts[0, column] + begin, limit)
        begin += extent
    named = jnp.where(lane < limit, lists_vec[...], -1).astype(jnp.float32)
    list_row[...] = jnp.full_like(list_row, -1.0)
    list_row[:, 0:LIST_LEN] = jnp.broadcast_to(named, (8, LIST_LEN))
    named = list_row[0:1, :]
    spot = lax.broadcasted_iota(jnp.int32, (1, 128), 1)
    first_z, first_y = 2 * CAP_X, 2 * CAP_X + 2 * CAP_Z
    offset = spot - first_z
    kept = BLOCKS + 2 * CAP_X + jnp.where(offset < CAP_Z, offset + CAP_Z, offset - CAP_Z)
    at_row = lax.broadcasted_iota(jnp.int32, (LIST_LEN, 128), 0)
    at_lane = lax.broadcasted_iota(jnp.int32, (LIST_LEN, 128), 1)
    tall = jnp.broadcast_to(named, (LIST_LEN, 128))
    tall = jnp.sum(jnp.where(at_row == at_lane, tall, 0.0), axis=1, keepdims=True)
    same = jnp.where(tall == kept.astype(jnp.float32), 1.0, 0.0)
    down = jnp.max(same[first_y : first_y + CAP_Y], axis=0, keepdims=True)
    up = jnp.max(same[first_y + CAP_Y :], axis=0, keepdims=True)
    note_send[...] = jnp.where(row == 0, 1.0 - down - up, jnp.where(row == 1, down, up))
    note_copies = [
        remote(at + 1, note_send, note_in.at[0], beside(gz=1)),
        remote(at + 2, note_send, note_in.at[1], beside(gz=-1)),
    ]
    at += 3

    total = mask.shape[1]
    block_id = lax.broadcasted_iota(jnp.int32, (total, 128), 0).astype(jnp.float32)
    hit = jnp.where(block_id == named, 1.0, 0.0)
    above = spot >= first_y + CAP_Y
    lists_of = (spot >= 0, (spot >= first_y) & jnp.logical_not(above), above)
    for c, lanes in enumerate(lists_of):
        found = jnp.max(jnp.where(lanes, hit, 0.0), axis=1, keepdims=True)
        if c == 0:
            found = 1.0 - found
        mask[c] = jnp.broadcast_to(found, (total, 128))

    tile = lax.broadcasted_iota(jnp.int32, (CELLS, 128), 0).astype(jnp.float32)

    def binned(blocks):
        hot, values = [], [[] for _ in blocks[0][2]]
        for block, place, weights in blocks:
            hot.append(jnp.where(tile == place, 1.0, 0.0).astype(jnp.bfloat16))
            high = block.astype(jnp.bfloat16).astype(jnp.float32)
            both = jnp.concatenate([high, block - high], axis=0)
            for c, weight in enumerate(weights):
                values[c].append((both * weight).astype(jnp.bfloat16))
        left = jnp.concatenate([jnp.concatenate(v, axis=1) for v in values], axis=0)
        right = jnp.concatenate(hot, axis=1)
        return lax.dot_general(
            left, right, (((1,), (1,)), ((), ())), preferred_element_type=jnp.float32
        )

    def weights_of(block):
        return [mask[c, pl.ds(block, 1), :] for c in range(3)]

    def whole(block, weights):
        return block, block[20:21], weights

    acc[0:144] = jnp.zeros((144, CELLS), jnp.float32)

    def own_group(group, _):
        start = group * GROUP
        acc[0:144] += binned(
            [whole(own[start + k], weights_of(start + k)) for k in range(GROUP)]
        )
        return 0

    lax.fori_loop(0, BLOCKS // GROUP, own_group, 0)
    near_copy.wait_recv()
    acc[0:144] += binned([whole(near_in[k], weights_of(near_id + k)) for k in range(CAP_X)])

    for copy in note_copies:
        copy.wait_recv()
    slot = lax.broadcasted_iota(jnp.int32, (16, 128), 0)
    here = lax.broadcasted_iota(jnp.int32, (16, 128), 1) == slot + first_z
    far_named = named == (row + far_id).astype(jnp.float32)
    for kind in range(3):
        kinds = [note_in[side, kind : kind + 1, :] for side in range(2)]
        found = jnp.where(here, jnp.where(slot < CAP_Z, kinds[0], kinds[1]), 0.0)
        found = jnp.max(found, axis=1, keepdims=True)
        slot_mask[kind] = jnp.broadcast_to(found, (16, 128))
        for side in range(2):
            begin = first_z + CAP_Z * side
            inside = (spot >= begin) & (spot < begin + CAP_Z)
            found = jnp.where(far_named & inside, kinds[side], 0.0)
            found = jnp.max(found, axis=1, keepdims=True)
            far_mask[3 * side + kind] = jnp.broadcast_to(found, (8, 128))
    for side in range(2):
        blocks = []
        for k in range(CAP_Z):
            entry = lists[0, first_z + CAP_Z * side + k]
            place = entry - near_id
            valid = k < counts[0, 2 + side]
            valid = valid & ((entry < BLOCKS) | ((place >= 0) & (place < CAP_X)))
            block = own[jnp.clip(entry, 0, BLOCKS - 1)]
            other = near_in[jnp.clip(place, 0, CAP_X - 1)]
            block = jnp.where(valid, jnp.where(entry < BLOCKS, block, other), 0.0)
            at_slot = CAP_Z * side + k
            weights = [slot_mask[c, at_slot : at_slot + 1, :] for c in range(3)]
            blocks.append(whole(block, weights))
        acc[144 * (1 + side) : 144 * (2 + side)] = binned(blocks)

    @pl.when(early & (gx != 0))
    def _():
        pl.semaphore_wait(ready, 1)
        for copy in far_copies:
            copy.start()

    for pair, copy in enumerate(far_copies):
        copy.wait_recv()
        first = 1 + 5 * pair
        last = far_in[first + 4]
        blocks = []
        for k, top in ((2 * pair, last), (2 * pair + 1, pltpu.roll(last, 4, 0))):
            start = first + 2 * (k % 2)
            block = jnp.concatenate([far_in[start], far_in[start + 1], top], axis=0)
            weights = weights_of(far_id + k)
            weights += [far_mask[c, k : k + 1, :] for c in range(6)]
            blocks.append((block, far_in[0, k : k + 1, :], weights))
        acc[...] += binned(blocks)

    def packed(dz, dy):
        first = 144 * CLASS[dz] + 48 * CLASS[dy]
        sums = acc[first : first + 24] + acc[first + 24 : first + 48]
        tiles = [sums[8 * r : 8 * r + 8, 128 * k : 128 * k + 128] for r in (0, 1) for k in range(4)]
        for k in (0, 256):
            pair = [sums[16:20, k : k + 128], sums[16:20, k + 128 : k + 256]]
            tiles.append(jnp.concatenate(pair, axis=0))
        return tiles

    sum_copies = []
    for m, (dz, dy) in enumerate(SENDS):
        for k, part in enumerate(packed(dz, dy)):
            sum_send[m, k] = part
        sum_copies.append(
            remote(at + m, sum_send.at[m], sum_in.at[m], beside(gz=dz, gy=dy))
        )

    @pl.when(gx == 0)
    def _():
        pl.semaphore_wait(ready, 1)
        for copy in far_copies:
            copy.start()

    result = packed(0, 0)
    for m, copy in enumerate(sum_copies):
        copy.wait_recv()
        result = [part + sum_in[m, k] for k, part in enumerate(result)]
    for k in range(4):
        columns = slice(128 * k, 128 * k + 128)
        out_ref[0:8, columns] = result[k]
        out_ref[8:16, columns] = result[4 + k]
        half = 4 * (k % 2)
        out_ref[16:20, columns] = result[8 + k // 2][half : half + 4]
    for copy in far_copies + [near_copy] + note_copies + sum_copies:
        copy.wait_send()


def solution(mesh):
    sizes = dict(mesh.shape)

    def per_device(particle_fields, step_length, live_mask, dest_cell, block_counts, block_lists):
        anywhere = pl.BlockSpec(memory_space=pl.ANY)
        copies = len(PARTS) + 3 + len(SENDS)
        return pl.pallas_call(
            functools.partial(kernel, sizes),
            out_shape=pltpu.VMEM((FIELDS, CELLS), jnp.float32),
            in_specs=[anywhere] * 6,
            out_specs=pl.BlockSpec(memory_space=pltpu.VMEM),
            scratch_shapes=[
                pltpu.VMEM((FIELDS, BLOCKS * 128), jnp.float32),
                pltpu.VMEM((BLOCKS, 128), jnp.float32),
                pltpu.VMEM((BLOCKS, 128), jnp.int32),
                pltpu.VMEM((BLOCKS, 128), jnp.int32),
                pltpu.SMEM((1, 6), jnp.int32),
                pltpu.SMEM((1, LIST_LEN), jnp.int32),
                pltpu.VMEM((1, LIST_LEN), jnp.int32),
                pltpu.VMEM((BLOCKS, ROWS, 128), jnp.float32),
                pltpu.VMEM((16, 8, 128), jnp.float32),
                pltpu.VMEM((CAP_X, ROWS, 128), jnp.float32),
                pltpu.VMEM((16, 8, 128), jnp.float32),
                pltpu.VMEM((CAP_X, ROWS, 128), jnp.float32),
                pltpu.VMEM((8, 128), jnp.float32),
                pltpu.VMEM((8, 128), jnp.float32),
                pltpu.VMEM((2, 8, 128), jnp.float32),
                pltpu.VMEM((len(SENDS), 10, 8, 128), jnp.float32),
                pltpu.VMEM((len(SENDS), 10, 8, 128), jnp.float32),
                pltpu.VMEM((3, BLOCKS + 16, 128), jnp.float32),
                pltpu.VMEM((6, 8, 128), jnp.float32),
                pltpu.VMEM((3, 16, 128), jnp.float32),
                pltpu.VMEM((9 * 2 * ROWS, CELLS), jnp.float32),
                pltpu.SemaphoreType.DMA((7,)),
                pltpu.SemaphoreType.DMA((copies,)),
                pltpu.SemaphoreType.DMA((copies,)),
                pltpu.SemaphoreType.REGULAR,
            ],
            compiler_params=pltpu.CompilerParams(collective_id=0, has_side_effects=True),
        )(
            particle_fields,
            step_length.reshape(BLOCKS, 128),
            live_mask.reshape(BLOCKS, 128),
            dest_cell.reshape(BLOCKS, 128),
            block_counts,
            block_lists,
        )

    placed = (P(None, AXES), P(AXES), P(AXES), P(AXES), P(AXES, None), P(AXES, None))
    return jax.shard_map(
        per_device, mesh=mesh, in_specs=placed, out_specs=P(None, AXES), check_vma=False
    )
```

```python
import functools

import jax
import jax.numpy as jnp
from jax import lax
from jax.experimental import pallas as pl
from jax.experimental.pallas import tpu as pltpu
from jax.sharding import PartitionSpec as P

MESH = pl.DeviceIdType.MESH
FIELDS = 20
BLOCKS = 64
CELLS = 512
CAP_X = 6
CAP_Z = 6
CAP_Y = 12
LIST_LEN = 48
ROWS = 24
GROUP = 8
LAG = 1
PARTS = ((0, 6), (6, 5), (11, 5))
SENDS = ((-1, 1), (1, 1), (-1, -1), (1, -1), (0, 1), (0, -1), (1, 0), (-1, 0))
CLASS = {0: 0, -1: 1, 1: 2}
AXES = ("gx", "gy", "gz")


def kernel(
    sizes,
    fields_hbm,
    step_hbm,
    live_hbm,
    cell_hbm,
    counts_hbm,
    lists_hbm,
    out_ref,
    fields,
    step,
    live,
    cell,
    counts,
    lists,
    lists_vec,
    own,
    far_send,
    near_send,
    far_in,
    near_in,
    list_row,
    note_send,
    note_in,
    sum_send,
    sum_in,
    mask,
    far_mask,
    slot_mask,
    acc,
    load_sem,
    send_sem,
    recv_sem,
    ready,
):
    def beside(**shifts):
        return {
            axis: lax.rem(lax.axis_index(axis) + shift + sizes[axis], sizes[axis])
            for axis, shift in shifts.items()
        }

    loads = [
        pltpu.make_async_copy(source, target, load_sem.at[k])
        for k, (source, target) in enumerate(
            (
                (lists_hbm, lists),
                (counts_hbm, counts),
                (lists_hbm, lists_vec),
                (step_hbm, step),
                (live_hbm, live),
                (cell_hbm, cell),
                (fields_hbm, fields),
            )
        )
    ]
    for load in loads:
        load.start()

    gx = lax.axis_index("gx")
    odd = lax.rem(gx, 2)
    toward_far = 2 * odd - 1
    early = (gx == 0) | ((odd == 1) & (gx != sizes["gx"] - 1))
    yields = (gx == sizes["gx"] - 1) & (lax.axis_index("gy") < 3 * sizes["gy"] // 4)
    barrier = pltpu.get_barrier_semaphore()

    def greet(where):
        pl.semaphore_signal(barrier, inc=1, device_id=where, device_id_type=MESH)

    greet(beside(gx=-toward_far))
    for dz, dy in SENDS:
        greet(beside(gz=dz, gy=dy))

    @pl.when(early)
    def _():
        greet(beside(gx=toward_far))

    far_slot, near_slot = CAP_X * odd, CAP_X * (1 - odd)
    far_id, near_id = BLOCKS + far_slot, BLOCKS + near_slot

    for load in loads:
        load.wait()

    row = lax.broadcasted_iota(jnp.int32, (8, 128), 0)

    def prepare(block, _):
        columns = pl.ds(pl.multiple_of(block * 128, 128), 128)
        one = pl.ds(block, 1)
        weight = jnp.broadcast_to(live[one, :].astype(jnp.float32), (8, 128))
        length = jnp.broadcast_to(step[one, :], (8, 128))
        place = jnp.broadcast_to(cell[one, :].astype(jnp.float32), (8, 128))
        first = fields[0:8, columns]
        moved = first + length * pltpu.roll(first, 5, 0)
        first = jnp.where(row < 3, moved, first)
        tail = jnp.where(row[0:4] == 0, place[0:4], 0.0)
        last = jnp.concatenate([fields[16:20, columns] * weight[0:4], tail], axis=0)
        own[block, 0:8, :] = first * weight
        own[block, 8:16, :] = fields[8:16, columns] * weight
        own[block, 16:24, :] = last
        return 0

    lax.fori_loop(0, BLOCKS, prepare, 0, unroll=8)

    tops, cells = [], jnp.zeros((8, 128), jnp.float32)
    for k in range(CAP_X):
        entry = jnp.clip(lists[0, far_slot + k], 0, BLOCKS - 1)
        block = jnp.where(k < counts[0, odd], own[entry], 0.0)
        tops.append(block[16:24])
        cells = jnp.where(row == k, block[20:21], cells)
        at = 1 + 5 * (k // 2) + 2 * (k % 2)
        far_send[at] = block[0:8]
        far_send[at + 1] = block[8:16]
        if k % 2:
            far_send[at + 2] = jnp.where(row < 4, tops[k - 1], pltpu.roll(tops[k], 4, 0))
    far_send[0] = cells
    for k in range(CAP_X):
        entry = jnp.clip(lists[0, near_slot + k], 0, BLOCKS - 1)
        near_send[k] = jnp.where(k < counts[0, 1 - odd], own[entry], 0.0)

    def describe(at, source, target, where):
        return pltpu.make_async_remote_copy(
            src_ref=source,
            dst_ref=target,
            send_sem=send_sem.at[at],
            recv_sem=recv_sem.at[at],
            device_id=where,
            device_id_type=MESH,
        )

    def remote(*what):
        copy = describe(*what)
        copy.start()
        return copy

    pl.semaphore_wait(barrier, jnp.where(early, len(SENDS) + 1, len(SENDS) + 2))
    far_copies = []
    for k, part in enumerate(PARTS):
        source, target = far_send.at[pl.ds(*part)], far_in.at[pl.ds(*part)]
        far_copies.append(describe(k, source, target, beside(gx=toward_far)))

    @pl.when(jnp.logical_not(early))
    def _():
        pl.semaphore_signal(
            ready, inc=1, device_id=beside(gx=toward_far), device_id_type=MESH
        )

    @pl.when(jnp.logical_not(early | yields))
    def _():
        for copy in far_copies:
            copy.start()

    at = len(PARTS)
    near_copy = remote(at, near_send, near_in, beside(gx=-toward_far))

    lane = lax.broadcasted_iota(jnp.int32, (1, LIST_LEN), 1)
    limit = jnp.zeros((1, LIST_LEN), jnp.int32)
    begin = 0
    for column, extent in enumerate((CAP_X, CAP_X, CAP_Z, CAP_Z, CAP_Y, CAP_Y)):
        inside = (lane >= begin) & (lane < begin + extent)
        limit = jnp.where(inside, counts[0, column] + begin, limit)
        begin += extent
    named = jnp.where(lane < limit, lists_vec[...], -1).astype(jnp.float32)
    list_row[...] = jnp.full_like(list_row, -1.0)
    list_row[:, 0:LIST_LEN] = jnp.broadcast_to(named, (8, LIST_LEN))
    named = list_row[0:1, :]
    spot = lax.broadcasted_iota(jnp.int32, (1, 128), 1)
    first_z, first_y = 2 * CAP_X, 2 * CAP_X + 2 * CAP_Z
    offset = spot - first_z
    kept = BLOCKS + 2 * CAP_X + jnp.where(offset < CAP_Z, offset + CAP_Z, offset - CAP_Z)
    at_row = lax.broadcasted_iota(jnp.int32, (LIST_LEN, 128), 0)
    at_lane = lax.broadcasted_iota(jnp.int32, (LIST_LEN, 128), 1)
    tall = jnp.broadcast_to(named, (LIST_LEN, 128))
    tall = jnp.sum(jnp.where(at_row == at_lane, tall, 0.0), axis=1, keepdims=True)
    same = jnp.where(tall == kept.astype(jnp.float32), 1.0, 0.0)
    down = jnp.max(same[first_y : first_y + CAP_Y], axis=0, keepdims=True)
    up = jnp.max(same[first_y + CAP_Y :], axis=0, keepdims=True)
    note_send[...] = jnp.where(row == 0, 1.0 - down - up, jnp.where(row == 1, down, up))
    note_copies = [
        remote(at + 1, note_send, note_in.at[0], beside(gz=1)),
        remote(at + 2, note_send, note_in.at[1], beside(gz=-1)),
    ]
    at += 3

    total = mask.shape[1]
    block_id = lax.broadcasted_iota(jnp.int32, (total, 128), 0).astype(jnp.float32)
    hit = jnp.where(block_id == named, 1.0, 0.0)
    above = spot >= first_y + CAP_Y
    lists_of = (spot >= 0, (spot >= first_y) & jnp.logical_not(above), above)
    for c, lanes in enumerate(lists_of):
        found = jnp.max(jnp.where(lanes, hit, 0.0), axis=1, keepdims=True)
        if c == 0:
            found = 1.0 - found
        mask[c] = jnp.broadcast_to(found, (total, 128))

    tile = lax.broadcasted_iota(jnp.int32, (CELLS, 128), 0).astype(jnp.float32)

    def binned(blocks):
        hot, values = [], [[] for _ in blocks[0][2]]
        for block, place, weights in blocks:
            hot.append(jnp.where(tile == place, 1.0, 0.0).astype(jnp.bfloat16))
            high = block.astype(jnp.bfloat16).astype(jnp.float32)
            both = jnp.concatenate([high, block - high], axis=0)
            for c, weight in enumerate(weights):
                values[c].append((both * weight).astype(jnp.bfloat16))
        left = jnp.concatenate([jnp.concatenate(v, axis=1) for v in values], axis=0)
        right = jnp.concatenate(hot, axis=1)
        return lax.dot_general(
            left, right, (((1,), (1,)), ((), ())), preferred_element_type=jnp.float32
        )

    def weights_of(block):
        return [mask[c, pl.ds(block, 1), :] for c in range(3)]

    def whole(block, weights):
        return block, block[20:21], weights

    acc[0:144] = jnp.zeros((144, CELLS), jnp.float32)

    def own_group(group, _):
        start = group * GROUP
        acc[0:144] += binned(
            [whole(own[start + k], weights_of(start + k)) for k in range(GROUP)]
        )
        return 0

    lax.fori_loop(0, LAG, own_group, 0)

    @pl.when(yields)
    def _():
        for copy in far_copies:
            copy.start()

    lax.fori_loop(LAG, BLOCKS // GROUP, own_group, 0)
    near_copy.wait_recv()
    acc[0:144] += binned([whole(near_in[k], weights_of(near_id + k)) for k in range(CAP_X)])

    for copy in note_copies:
        copy.wait_recv()
    slot = lax.broadcasted_iota(jnp.int32, (16, 128), 0)
    here = lax.broadcasted_iota(jnp.int32, (16, 128), 1) == slot + first_z
    far_named = named == (row + far_id).astype(jnp.float32)
    for kind in range(3):
        kinds = [note_in[side, kind : kind + 1, :] for side in range(2)]
        found = jnp.where(here, jnp.where(slot < CAP_Z, kinds[0], kinds[1]), 0.0)
        found = jnp.max(found, axis=1, keepdims=True)
        slot_mask[kind] = jnp.broadcast_to(found, (16, 128))
        for side in range(2):
            begin = first_z + CAP_Z * side
            inside = (spot >= begin) & (spot < begin + CAP_Z)
            found = jnp.where(far_named & inside, kinds[side], 0.0)
            found = jnp.max(found, axis=1, keepdims=True)
            far_mask[3 * side + kind] = jnp.broadcast_to(found, (8, 128))
    for side in range(2):
        blocks = []
        for k in range(CAP_Z):
            entry = lists[0, first_z + CAP_Z * side + k]
            place = entry - near_id
            valid = k < counts[0, 2 + side]
            valid = valid & ((entry < BLOCKS) | ((place >= 0) & (place < CAP_X)))
            block = own[jnp.clip(entry, 0, BLOCKS - 1)]
            other = near_in[jnp.clip(place, 0, CAP_X - 1)]
            block = jnp.where(valid, jnp.where(entry < BLOCKS, block, other), 0.0)
            at_slot = CAP_Z * side + k
            weights = [slot_mask[c, at_slot : at_slot + 1, :] for c in range(3)]
            blocks.append(whole(block, weights))
        acc[144 * (1 + side) : 144 * (2 + side)] = binned(blocks)

    @pl.when(early & (gx != 0))
    def _():
        pl.semaphore_wait(ready, 1)
        for copy in far_copies:
            copy.start()

    for pair, copy in enumerate(far_copies):
        copy.wait_recv()
        first = 1 + 5 * pair
        last = far_in[first + 4]
        blocks = []
        for k, top in ((2 * pair, last), (2 * pair + 1, pltpu.roll(last, 4, 0))):
            start = first + 2 * (k % 2)
            block = jnp.concatenate([far_in[start], far_in[start + 1], top], axis=0)
            weights = weights_of(far_id + k)
            weights += [far_mask[c, k : k + 1, :] for c in range(6)]
            blocks.append((block, far_in[0, k : k + 1, :], weights))
        acc[...] += binned(blocks)

    def packed(dz, dy):
        first = 144 * CLASS[dz] + 48 * CLASS[dy]
        sums = acc[first : first + 24] + acc[first + 24 : first + 48]
        tiles = [sums[8 * r : 8 * r + 8, 128 * k : 128 * k + 128] for r in (0, 1) for k in range(4)]
        for k in (0, 256):
            pair = [sums[16:20, k : k + 128], sums[16:20, k + 128 : k + 256]]
            tiles.append(jnp.concatenate(pair, axis=0))
        return tiles

    sum_copies = []
    for m, (dz, dy) in enumerate(SENDS):
        for k, part in enumerate(packed(dz, dy)):
            sum_send[m, k] = part
        sum_copies.append(
            remote(at + m, sum_send.at[m], sum_in.at[m], beside(gz=dz, gy=dy))
        )

    @pl.when(gx == 0)
    def _():
        pl.semaphore_wait(ready, 1)
        for copy in far_copies:
            copy.start()

    result = packed(0, 0)
    for m, copy in enumerate(sum_copies):
        copy.wait_recv()
        result = [part + sum_in[m, k] for k, part in enumerate(result)]
    for k in range(4):
        columns = slice(128 * k, 128 * k + 128)
        out_ref[0:8, columns] = result[k]
        out_ref[8:16, columns] = result[4 + k]
        half = 4 * (k % 2)
        out_ref[16:20, columns] = result[8 + k // 2][half : half + 4]
    for copy in far_copies + [near_copy] + note_copies + sum_copies:
        copy.wait_send()


def solution(mesh):
    sizes = dict(mesh.shape)

    def per_device(particle_fields, step_length, live_mask, dest_cell, block_counts, block_lists):
        anywhere = pl.BlockSpec(memory_space=pl.ANY)
        copies = len(PARTS) + 3 + len(SENDS)
        return pl.pallas_call(
            functools.partial(kernel, sizes),
            out_shape=pltpu.VMEM((FIELDS, CELLS), jnp.float32),
            in_specs=[anywhere] * 6,
            out_specs=pl.BlockSpec(memory_space=pltpu.VMEM),
            scratch_shapes=[
                pltpu.VMEM((FIELDS, BLOCKS * 128), jnp.float32),
                pltpu.VMEM((BLOCKS, 128), jnp.float32),
                pltpu.VMEM((BLOCKS, 128), jnp.int32),
                pltpu.VMEM((BLOCKS, 128), jnp.int32),
                pltpu.SMEM((1, 6), jnp.int32),
                pltpu.SMEM((1, LIST_LEN), jnp.int32),
                pltpu.VMEM((1, LIST_LEN), jnp.int32),
                pltpu.VMEM((BLOCKS, ROWS, 128), jnp.float32),
                pltpu.VMEM((16, 8, 128), jnp.float32),
                pltpu.VMEM((CAP_X, ROWS, 128), jnp.float32),
                pltpu.VMEM((16, 8, 128), jnp.float32),
                pltpu.VMEM((CAP_X, ROWS, 128), jnp.float32),
                pltpu.VMEM((8, 128), jnp.float32),
                pltpu.VMEM((8, 128), jnp.float32),
                pltpu.VMEM((2, 8, 128), jnp.float32),
                pltpu.VMEM((len(SENDS), 10, 8, 128), jnp.float32),
                pltpu.VMEM((len(SENDS), 10, 8, 128), jnp.float32),
                pltpu.VMEM((3, BLOCKS + 16, 128), jnp.float32),
                pltpu.VMEM((6, 8, 128), jnp.float32),
                pltpu.VMEM((3, 16, 128), jnp.float32),
                pltpu.VMEM((9 * 2 * ROWS, CELLS), jnp.float32),
                pltpu.SemaphoreType.DMA((7,)),
                pltpu.SemaphoreType.DMA((copies,)),
                pltpu.SemaphoreType.DMA((copies,)),
                pltpu.SemaphoreType.REGULAR,
            ],
            compiler_params=pltpu.CompilerParams(collective_id=0, has_side_effects=True),
        )(
            particle_fields,
            step_length.reshape(BLOCKS, 128),
            live_mask.reshape(BLOCKS, 128),
            dest_cell.reshape(BLOCKS, 128),
            block_counts,
            block_lists,
        )

    placed = (P(None, AXES), P(AXES), P(AXES), P(AXES), P(AXES, None), P(AXES, None))
    return jax.shard_map(
        per_device, mesh=mesh, in_specs=placed, out_specs=P(None, AXES), check_vma=False
    )
```

```python
import functools

import jax
import jax.numpy as jnp
from jax import lax
from jax.experimental import pallas as pl
from jax.experimental.pallas import tpu as pltpu
from jax.sharding import PartitionSpec as P

MESH = pl.DeviceIdType.MESH
FIELDS = 20
BLOCKS = 64
CELLS = 512
CAP_X = 6
CAP_Z = 6
CAP_Y = 12
LIST_LEN = 48
ROWS = 24
GROUP = 8
LAG = 2
PARTS = ((0, 6), (6, 5), (11, 5))
SENDS = ((-1, 1), (1, 1), (-1, -1), (1, -1), (0, 1), (0, -1), (1, 0), (-1, 0))
CLASS = {0: 0, -1: 1, 1: 2}
AXES = ("gx", "gy", "gz")


def kernel(
    sizes,
    fields_hbm,
    step_hbm,
    live_hbm,
    cell_hbm,
    counts_hbm,
    lists_hbm,
    out_ref,
    fields,
    step,
    live,
    cell,
    counts,
    lists,
    lists_vec,
    own,
    far_send,
    near_send,
    far_in,
    near_in,
    list_row,
    note_send,
    note_in,
    sum_send,
    sum_in,
    mask,
    far_mask,
    slot_mask,
    acc,
    load_sem,
    send_sem,
    recv_sem,
    ready,
    near_ok,
    passed_on,
    all_in,
):
    def beside(**shifts):
        return {
            axis: lax.rem(lax.axis_index(axis) + shift + sizes[axis], sizes[axis])
            for axis, shift in shifts.items()
        }

    loads = [
        pltpu.make_async_copy(source, target, load_sem.at[k])
        for k, (source, target) in enumerate(
            (
                (lists_hbm, lists),
                (counts_hbm, counts),
                (lists_hbm, lists_vec),
                (step_hbm, step),
                (live_hbm, live),
                (cell_hbm, cell),
                (fields_hbm, fields),
            )
        )
    ]
    for load in loads:
        load.start()

    gx = lax.axis_index("gx")
    odd = lax.rem(gx, 2)
    toward_far = 2 * odd - 1
    early = (gx == 0) | ((odd == 1) & (gx != sizes["gx"] - 1))
    barrier = pltpu.get_barrier_semaphore()

    def greet(where):
        pl.semaphore_signal(barrier, inc=1, device_id=where, device_id_type=MESH)

    last_row = gx == sizes["gx"] - 1
    by_last = gx == sizes["gx"] - 2

    @pl.when(jnp.logical_not(by_last))
    def _():
        greet(beside(gx=-toward_far))

    @pl.when(jnp.logical_not(last_row))
    def _():
        for dz, dy in SENDS:
            greet(beside(gz=dz, gy=dy))


    @pl.when(early)
    def _():
        greet(beside(gx=toward_far))

    yields = last_row & (lax.axis_index("gy") < 3 * sizes["gy"] // 4)

    far_slot, near_slot = CAP_X * odd, CAP_X * (1 - odd)
    far_id, near_id = BLOCKS + far_slot, BLOCKS + near_slot

    for load in loads:
        load.wait()

    row = lax.broadcasted_iota(jnp.int32, (8, 128), 0)

    def prepare(block, _):
        columns = pl.ds(pl.multiple_of(block * 128, 128), 128)
        one = pl.ds(block, 1)
        weight = jnp.broadcast_to(live[one, :].astype(jnp.float32), (8, 128))
        length = jnp.broadcast_to(step[one, :], (8, 128))
        place = jnp.broadcast_to(cell[one, :].astype(jnp.float32), (8, 128))
        first = fields[0:8, columns]
        moved = first + length * pltpu.roll(first, 5, 0)
        first = jnp.where(row < 3, moved, first)
        tail = jnp.where(row[0:4] == 0, place[0:4], 0.0)
        last = jnp.concatenate([fields[16:20, columns] * weight[0:4], tail], axis=0)
        own[block, 0:8, :] = first * weight
        own[block, 8:16, :] = fields[8:16, columns] * weight
        own[block, 16:24, :] = last
        return 0

    lax.fori_loop(0, BLOCKS, prepare, 0, unroll=8)

    tops, cells = [], jnp.zeros((8, 128), jnp.float32)
    for k in range(CAP_X):
        entry = jnp.clip(lists[0, far_slot + k], 0, BLOCKS - 1)
        block = jnp.where(k < counts[0, odd], own[entry], 0.0)
        tops.append(block[16:24])
        cells = jnp.where(row == k, block[20:21], cells)
        at = 1 + 5 * (k // 2) + 2 * (k % 2)
        far_send[at] = block[0:8]
        far_send[at + 1] = block[8:16]
        if k % 2:
            far_send[at + 2] = jnp.where(row < 4, tops[k - 1], pltpu.roll(tops[k], 4, 0))
    far_send[0] = cells
    for k in range(CAP_X):
        entry = jnp.clip(lists[0, near_slot + k], 0, BLOCKS - 1)
        near_send[k] = jnp.where(k < counts[0, 1 - odd], own[entry], 0.0)

    def describe(at, source, target, where):
        return pltpu.make_async_remote_copy(
            src_ref=source,
            dst_ref=target,
            send_sem=send_sem.at[at],
            recv_sem=recv_sem.at[at],
            device_id=where,
            device_id_type=MESH,
        )

    def remote(*what):
        copy = describe(*what)
        copy.start()
        return copy

    greeted = jnp.where(early, len(SENDS) + 1, len(SENDS) + 2)
    pl.semaphore_wait(barrier, jnp.where(last_row, 1, greeted))
    far_copies = []
    for k, part in enumerate(PARTS):
        source, target = far_send.at[pl.ds(*part)], far_in.at[pl.ds(*part)]
        far_copies.append(describe(k, source, target, beside(gx=toward_far)))

    @pl.when(jnp.logical_not(early))
    def _():
        pl.semaphore_signal(
            ready, inc=1, device_id=beside(gx=toward_far), device_id_type=MESH
        )

    @pl.when(jnp.logical_not(early | yields))
    def _():
        for copy in far_copies:
            copy.start()

    at = len(PARTS)
    near_copy = describe(at, near_send, near_in, beside(gx=-toward_far))

    @pl.when(jnp.logical_not(last_row))
    def _():
        near_copy.start()

    @pl.when(by_last)
    def _():
        pl.semaphore_signal(
            near_ok, inc=1, device_id=beside(gx=-toward_far), device_id_type=MESH
        )


    lane = lax.broadcasted_iota(jnp.int32, (1, LIST_LEN), 1)
    limit = jnp.zeros((1, LIST_LEN), jnp.int32)
    begin = 0
    for column, extent in enumerate((CAP_X, CAP_X, CAP_Z, CAP_Z, CAP_Y, CAP_Y)):
        inside = (lane >= begin) & (lane < begin + extent)
        limit = jnp.where(inside, counts[0, column] + begin, limit)
        begin += extent
    named = jnp.where(lane < limit, lists_vec[...], -1).astype(jnp.float32)
    list_row[...] = jnp.full_like(list_row, -1.0)
    list_row[:, 0:LIST_LEN] = jnp.broadcast_to(named, (8, LIST_LEN))
    named = list_row[0:1, :]
    spot = lax.broadcasted_iota(jnp.int32, (1, 128), 1)
    first_z, first_y = 2 * CAP_X, 2 * CAP_X + 2 * CAP_Z
    offset = spot - first_z
    kept = BLOCKS + 2 * CAP_X + jnp.where(offset < CAP_Z, offset + CAP_Z, offset - CAP_Z)
    at_row = lax.broadcasted_iota(jnp.int32, (LIST_LEN, 128), 0)
    at_lane = lax.broadcasted_iota(jnp.int32, (LIST_LEN, 128), 1)
    tall = jnp.broadcast_to(named, (LIST_LEN, 128))
    tall = jnp.sum(jnp.where(at_row == at_lane, tall, 0.0), axis=1, keepdims=True)
    same = jnp.where(tall == kept.astype(jnp.float32), 1.0, 0.0)
    down = jnp.max(same[first_y : first_y + CAP_Y], axis=0, keepdims=True)
    up = jnp.max(same[first_y + CAP_Y :], axis=0, keepdims=True)
    note_send[...] = jnp.where(row == 0, 1.0 - down - up, jnp.where(row == 1, down, up))
    note_copies = [
        describe(at + 1, note_send, note_in.at[0], beside(gz=1)),
        describe(at + 2, note_send, note_in.at[1], beside(gz=-1)),
    ]

    @pl.when(jnp.logical_not(last_row))
    def _():
        for copy in note_copies:
            copy.start()

    at += 3

    total = mask.shape[1]
    block_id = lax.broadcasted_iota(jnp.int32, (total, 128), 0).astype(jnp.float32)
    hit = jnp.where(block_id == named, 1.0, 0.0)
    above = spot >= first_y + CAP_Y
    lists_of = (spot >= 0, (spot >= first_y) & jnp.logical_not(above), above)
    for c, lanes in enumerate(lists_of):
        found = jnp.max(jnp.where(lanes, hit, 0.0), axis=1, keepdims=True)
        if c == 0:
            found = 1.0 - found
        mask[c] = jnp.broadcast_to(found, (total, 128))

    tile = lax.broadcasted_iota(jnp.int32, (CELLS, 128), 0).astype(jnp.float32)

    def binned(blocks):
        hot, values = [], [[] for _ in blocks[0][2]]
        for block, place, weights in blocks:
            hot.append(jnp.where(tile == place, 1.0, 0.0).astype(jnp.bfloat16))
            high = block.astype(jnp.bfloat16).astype(jnp.float32)
            both = jnp.concatenate([high, block - high], axis=0)
            for c, weight in enumerate(weights):
                values[c].append((both * weight).astype(jnp.bfloat16))
        left = jnp.concatenate([jnp.concatenate(v, axis=1) for v in values], axis=0)
        right = jnp.concatenate(hot, axis=1)
        return lax.dot_general(
            left, right, (((1,), (1,)), ((), ())), preferred_element_type=jnp.float32
        )

    def weights_of(block):
        return [mask[c, pl.ds(block, 1), :] for c in range(3)]

    def whole(block, weights):
        return block, block[20:21], weights

    acc[0:144] = jnp.zeros((144, CELLS), jnp.float32)

    def own_group(group, _):
        start = group * GROUP
        acc[0:144] += binned(
            [whole(own[start + k], weights_of(start + k)) for k in range(GROUP)]
        )
        return 0

    lax.fori_loop(0, LAG, own_group, 0)

    @pl.when(yields)
    def _():
        for copy in far_copies:
            copy.start()

    lax.fori_loop(LAG, BLOCKS // GROUP, own_group, 0)

    @pl.when(last_row)
    def _():
        pl.semaphore_wait(near_ok, 1)
        near_copy.start()

    near_copy.wait_recv()
    acc[0:144] += binned([whole(near_in[k], weights_of(near_id + k)) for k in range(CAP_X)])

    @pl.when(last_row)
    def _():
        pl.semaphore_wait(all_in, 1)
        for copy in note_copies:
            copy.start()

    for copy in note_copies:
        copy.wait_recv()
    slot = lax.broadcasted_iota(jnp.int32, (16, 128), 0)
    here = lax.broadcasted_iota(jnp.int32, (16, 128), 1) == slot + first_z
    far_named = named == (row + far_id).astype(jnp.float32)
    for kind in range(3):
        kinds = [note_in[side, kind : kind + 1, :] for side in range(2)]
        found = jnp.where(here, jnp.where(slot < CAP_Z, kinds[0], kinds[1]), 0.0)
        found = jnp.max(found, axis=1, keepdims=True)
        slot_mask[kind] = jnp.broadcast_to(found, (16, 128))
        for side in range(2):
            begin = first_z + CAP_Z * side
            inside = (spot >= begin) & (spot < begin + CAP_Z)
            found = jnp.where(far_named & inside, kinds[side], 0.0)
            found = jnp.max(found, axis=1, keepdims=True)
            far_mask[3 * side + kind] = jnp.broadcast_to(found, (8, 128))
    for side in range(2):
        blocks = []
        for k in range(CAP_Z):
            entry = lists[0, first_z + CAP_Z * side + k]
            place = entry - near_id
            valid = k < counts[0, 2 + side]
            valid = valid & ((entry < BLOCKS) | ((place >= 0) & (place < CAP_X)))
            block = own[jnp.clip(entry, 0, BLOCKS - 1)]
            other = near_in[jnp.clip(place, 0, CAP_X - 1)]
            block = jnp.where(valid, jnp.where(entry < BLOCKS, block, other), 0.0)
            at_slot = CAP_Z * side + k
            weights = [slot_mask[c, at_slot : at_slot + 1, :] for c in range(3)]
            blocks.append(whole(block, weights))
        acc[144 * (1 + side) : 144 * (2 + side)] = binned(blocks)

    @pl.when(gx == 0)
    def _():
        pl.semaphore_wait(ready, 1)
        for dz, dy in SENDS:
            pl.semaphore_signal(
                passed_on, inc=1, device_id=beside(gz=dz, gy=dy), device_id_type=MESH
            )

    @pl.when(early & (gx != 0))
    def _():
        pl.semaphore_wait(ready, 1)
        for copy in far_copies:
            copy.start()

    for pair, copy in enumerate(far_copies):
        copy.wait_recv()
        first = 1 + 5 * pair
        last = far_in[first + 4]
        blocks = []
        for k, top in ((2 * pair, last), (2 * pair + 1, pltpu.roll(last, 4, 0))):
            start = first + 2 * (k % 2)
            block = jnp.concatenate([far_in[start], far_in[start + 1], top], axis=0)
            weights = weights_of(far_id + k)
            weights += [far_mask[c, k : k + 1, :] for c in range(6)]
            blocks.append((block, far_in[0, k : k + 1, :], weights))
        acc[...] += binned(blocks)

    def packed(dz, dy):
        first = 144 * CLASS[dz] + 48 * CLASS[dy]
        sums = acc[first : first + 24] + acc[first + 24 : first + 48]
        tiles = [sums[8 * r : 8 * r + 8, 128 * k : 128 * k + 128] for r in (0, 1) for k in range(4)]
        for k in (0, 256):
            pair = [sums[16:20, k : k + 128], sums[16:20, k + 128 : k + 256]]
            tiles.append(jnp.concatenate(pair, axis=0))
        return tiles

    sum_copies = []
    for m, (dz, dy) in enumerate(SENDS):
        for k, part in enumerate(packed(dz, dy)):
            sum_send[m, k] = part
        sum_copies.append(
            remote(at + m, sum_send.at[m], sum_in.at[m], beside(gz=dz, gy=dy))
        )

    @pl.when(gx == 0)
    def _():
        for copy in far_copies:
            copy.start()
        pl.semaphore_wait(passed_on, len(SENDS))
        pl.semaphore_signal(
            all_in, inc=1, device_id=beside(gx=toward_far), device_id_type=MESH
        )

    result = packed(0, 0)
    for m, copy in enumerate(sum_copies):
        copy.wait_recv()
        result = [part + sum_in[m, k] for k, part in enumerate(result)]
    for k in range(4):
        columns = slice(128 * k, 128 * k + 128)
        out_ref[0:8, columns] = result[k]
        out_ref[8:16, columns] = result[4 + k]
        half = 4 * (k % 2)
        out_ref[16:20, columns] = result[8 + k // 2][half : half + 4]
    for copy in far_copies + [near_copy] + note_copies + sum_copies:
        copy.wait_send()


def solution(mesh):
    sizes = dict(mesh.shape)

    def per_device(particle_fields, step_length, live_mask, dest_cell, block_counts, block_lists):
        anywhere = pl.BlockSpec(memory_space=pl.ANY)
        copies = len(PARTS) + 3 + len(SENDS)
        return pl.pallas_call(
            functools.partial(kernel, sizes),
            out_shape=pltpu.VMEM((FIELDS, CELLS), jnp.float32),
            in_specs=[anywhere] * 6,
            out_specs=pl.BlockSpec(memory_space=pltpu.VMEM),
            scratch_shapes=[
                pltpu.VMEM((FIELDS, BLOCKS * 128), jnp.float32),
                pltpu.VMEM((BLOCKS, 128), jnp.float32),
                pltpu.VMEM((BLOCKS, 128), jnp.int32),
                pltpu.VMEM((BLOCKS, 128), jnp.int32),
                pltpu.SMEM((1, 6), jnp.int32),
                pltpu.SMEM((1, LIST_LEN), jnp.int32),
                pltpu.VMEM((1, LIST_LEN), jnp.int32),
                pltpu.VMEM((BLOCKS, ROWS, 128), jnp.float32),
                pltpu.VMEM((16, 8, 128), jnp.float32),
                pltpu.VMEM((CAP_X, ROWS, 128), jnp.float32),
                pltpu.VMEM((16, 8, 128), jnp.float32),
                pltpu.VMEM((CAP_X, ROWS, 128), jnp.float32),
                pltpu.VMEM((8, 128), jnp.float32),
                pltpu.VMEM((8, 128), jnp.float32),
                pltpu.VMEM((2, 8, 128), jnp.float32),
                pltpu.VMEM((len(SENDS), 10, 8, 128), jnp.float32),
                pltpu.VMEM((len(SENDS), 10, 8, 128), jnp.float32),
                pltpu.VMEM((3, BLOCKS + 16, 128), jnp.float32),
                pltpu.VMEM((6, 8, 128), jnp.float32),
                pltpu.VMEM((3, 16, 128), jnp.float32),
                pltpu.VMEM((9 * 2 * ROWS, CELLS), jnp.float32),
                pltpu.SemaphoreType.DMA((7,)),
                pltpu.SemaphoreType.DMA((copies,)),
                pltpu.SemaphoreType.DMA((copies,)),
                pltpu.SemaphoreType.REGULAR,
                pltpu.SemaphoreType.REGULAR,
                pltpu.SemaphoreType.REGULAR,
                pltpu.SemaphoreType.REGULAR,
            ],
            compiler_params=pltpu.CompilerParams(collective_id=0, has_side_effects=True),
        )(
            particle_fields,
            step_length.reshape(BLOCKS, 128),
            live_mask.reshape(BLOCKS, 128),
            dest_cell.reshape(BLOCKS, 128),
            block_counts,
            block_lists,
        )

    placed = (P(None, AXES), P(AXES), P(AXES), P(AXES), P(AXES, None), P(AXES, None))
    return jax.shard_map(
        per_device, mesh=mesh, in_specs=placed, out_specs=P(None, AXES), check_vma=False
    )
```

```python
import functools

import jax
import jax.numpy as jnp
from jax import lax
from jax.experimental import pallas as pl
from jax.experimental.pallas import tpu as pltpu
from jax.sharding import PartitionSpec as P

MESH = pl.DeviceIdType.MESH
FIELDS = 20
BLOCKS = 64
CELLS = 512
CAP_X = 6
CAP_Z = 6
CAP_Y = 12
LIST_LEN = 48
ROWS = 24
GROUP = 8
LAG = 2
PARTS = ((0, 6), (6, 5), (11, 5))
SENDS = ((-1, 1), (1, 1), (-1, -1), (1, -1), (0, 1), (0, -1), (1, 0), (-1, 0))
CLASS = {0: 0, -1: 1, 1: 2}
AXES = ("gx", "gy", "gz")


def kernel(
    sizes,
    fields_hbm,
    step_hbm,
    live_hbm,
    cell_hbm,
    counts_hbm,
    lists_hbm,
    out_ref,
    fields,
    step,
    live,
    cell,
    counts,
    lists,
    lists_vec,
    own,
    far_send,
    near_send,
    far_in,
    near_in,
    list_row,
    note_send,
    note_in,
    sum_send,
    sum_in,
    mask,
    far_mask,
    slot_mask,
    acc,
    load_sem,
    send_sem,
    recv_sem,
    ready,
    near_ok,
    passed_on,
    all_in,
):
    def beside(**shifts):
        return {
            axis: lax.rem(lax.axis_index(axis) + shift + sizes[axis], sizes[axis])
            for axis, shift in shifts.items()
        }

    quarters = [pl.ds(16 * 128 * k, 16 * 128) for k in range(4)]
    loads = [
        pltpu.make_async_copy(source, target, load_sem.at[k])
        for k, (source, target) in enumerate(
            (
                *((fields_hbm.at[:, q], fields.at[:, q]) for q in quarters),
                (lists_hbm, lists),
                (counts_hbm, counts),
                (lists_hbm, lists_vec),
                (step_hbm, step),
                (live_hbm, live),
                (cell_hbm, cell),
            )
        )
    ]
    for load in loads:
        load.start()

    gx = lax.axis_index("gx")
    odd = lax.rem(gx, 2)
    toward_far = 2 * odd - 1
    early = (gx == 0) | ((odd == 1) & (gx != sizes["gx"] - 1))
    barrier = pltpu.get_barrier_semaphore()

    def greet(where):
        pl.semaphore_signal(barrier, inc=1, device_id=where, device_id_type=MESH)

    last_row = gx == sizes["gx"] - 1
    by_last = gx == sizes["gx"] - 2

    @pl.when(jnp.logical_not(by_last))
    def _():
        greet(beside(gx=-toward_far))

    @pl.when(jnp.logical_not(last_row))
    def _():
        for dz, dy in SENDS:
            greet(beside(gz=dz, gy=dy))


    @pl.when(early)
    def _():
        greet(beside(gx=toward_far))

    yields = last_row & (lax.axis_index("gy") < 3 * sizes["gy"] // 4)

    far_slot, near_slot = CAP_X * odd, CAP_X * (1 - odd)
    far_id, near_id = BLOCKS + far_slot, BLOCKS + near_slot

    for load in loads:
        load.wait()

    row = lax.broadcasted_iota(jnp.int32, (8, 128), 0)

    def prepare(block, _):
        columns = pl.ds(pl.multiple_of(block * 128, 128), 128)
        one = pl.ds(block, 1)
        weight = jnp.broadcast_to(live[one, :].astype(jnp.float32), (8, 128))
        length = jnp.broadcast_to(step[one, :], (8, 128))
        place = jnp.broadcast_to(cell[one, :].astype(jnp.float32), (8, 128))
        first = fields[0:8, columns]
        moved = first + length * pltpu.roll(first, 5, 0)
        first = jnp.where(row < 3, moved, first)
        tail = jnp.where(row[0:4] == 0, place[0:4], 0.0)
        last = jnp.concatenate([fields[16:20, columns] * weight[0:4], tail], axis=0)
        own[block, 0:8, :] = first * weight
        own[block, 8:16, :] = fields[8:16, columns] * weight
        own[block, 16:24, :] = last
        return 0

    lax.fori_loop(0, BLOCKS, prepare, 0, unroll=16)

    tops, cells = [], jnp.zeros((8, 128), jnp.float32)
    for k in range(CAP_X):
        entry = jnp.clip(lists[0, far_slot + k], 0, BLOCKS - 1)
        block = jnp.where(k < counts[0, odd], own[entry], 0.0)
        tops.append(block[16:24])
        cells = jnp.where(row == k, block[20:21], cells)
        at = 1 + 5 * (k // 2) + 2 * (k % 2)
        far_send[at] = block[0:8]
        far_send[at + 1] = block[8:16]
        if k % 2:
            far_send[at + 2] = jnp.where(row < 4, tops[k - 1], pltpu.roll(tops[k], 4, 0))
    far_send[0] = cells
    def describe(at, source, target, where):
        return pltpu.make_async_remote_copy(
            src_ref=source,
            dst_ref=target,
            send_sem=send_sem.at[at],
            recv_sem=recv_sem.at[at],
            device_id=where,
            device_id_type=MESH,
        )

    def remote(*what):
        copy = describe(*what)
        copy.start()
        return copy

    greeted = jnp.where(early, len(SENDS) + 1, len(SENDS) + 2)
    pl.semaphore_wait(barrier, jnp.where(last_row, 1, greeted))
    far_copies = []
    for k, part in enumerate(PARTS):
        source, target = far_send.at[pl.ds(*part)], far_in.at[pl.ds(*part)]
        far_copies.append(describe(k, source, target, beside(gx=toward_far)))

    @pl.when(jnp.logical_not(early))
    def _():
        pl.semaphore_signal(
            ready, inc=1, device_id=beside(gx=toward_far), device_id_type=MESH
        )

    @pl.when(jnp.logical_not(early | yields))
    def _():
        for copy in far_copies:
            copy.start()

    at = len(PARTS)
    for k in range(CAP_X):
        entry = jnp.clip(lists[0, near_slot + k], 0, BLOCKS - 1)
        near_send[k] = jnp.where(k < counts[0, 1 - odd], own[entry], 0.0)

    near_copy = describe(at, near_send, near_in, beside(gx=-toward_far))

    @pl.when(jnp.logical_not(last_row))
    def _():
        near_copy.start()

    @pl.when(by_last)
    def _():
        pl.semaphore_signal(
            near_ok, inc=1, device_id=beside(gx=-toward_far), device_id_type=MESH
        )


    lane = lax.broadcasted_iota(jnp.int32, (1, LIST_LEN), 1)
    limit = jnp.zeros((1, LIST_LEN), jnp.int32)
    begin = 0
    for column, extent in enumerate((CAP_X, CAP_X, CAP_Z, CAP_Z, CAP_Y, CAP_Y)):
        inside = (lane >= begin) & (lane < begin + extent)
        limit = jnp.where(inside, counts[0, column] + begin, limit)
        begin += extent
    named = jnp.where(lane < limit, lists_vec[...], -1).astype(jnp.float32)
    list_row[...] = jnp.full_like(list_row, -1.0)
    list_row[:, 0:LIST_LEN] = jnp.broadcast_to(named, (8, LIST_LEN))
    named = list_row[0:1, :]
    spot = lax.broadcasted_iota(jnp.int32, (1, 128), 1)
    first_z, first_y = 2 * CAP_X, 2 * CAP_X + 2 * CAP_Z
    offset = spot - first_z
    kept = BLOCKS + 2 * CAP_X + jnp.where(offset < CAP_Z, offset + CAP_Z, offset - CAP_Z)
    at_row = lax.broadcasted_iota(jnp.int32, (LIST_LEN, 128), 0)
    at_lane = lax.broadcasted_iota(jnp.int32, (LIST_LEN, 128), 1)
    tall = jnp.broadcast_to(named, (LIST_LEN, 128))
    tall = jnp.sum(jnp.where(at_row == at_lane, tall, 0.0), axis=1, keepdims=True)
    same = jnp.where(tall == kept.astype(jnp.float32), 1.0, 0.0)
    down = jnp.max(same[first_y : first_y + CAP_Y], axis=0, keepdims=True)
    up = jnp.max(same[first_y + CAP_Y :], axis=0, keepdims=True)
    note_send[...] = jnp.where(row == 0, 1.0 - down - up, jnp.where(row == 1, down, up))
    note_copies = [
        describe(at + 1, note_send, note_in.at[0], beside(gz=1)),
        describe(at + 2, note_send, note_in.at[1], beside(gz=-1)),
    ]

    @pl.when(jnp.logical_not(last_row))
    def _():
        for copy in note_copies:
            copy.start()

    at += 3

    total = mask.shape[1]
    block_id = lax.broadcasted_iota(jnp.int32, (total, 128), 0).astype(jnp.float32)
    hit = jnp.where(block_id == named, 1.0, 0.0)
    above = spot >= first_y + CAP_Y
    lists_of = (spot >= 0, (spot >= first_y) & jnp.logical_not(above), above)
    for c, lanes in enumerate(lists_of):
        found = jnp.max(jnp.where(lanes, hit, 0.0), axis=1, keepdims=True)
        if c == 0:
            found = 1.0 - found
        mask[c] = jnp.broadcast_to(found, (total, 128))

    tile = lax.broadcasted_iota(jnp.int32, (CELLS, 128), 0).astype(jnp.float32)

    def binned(blocks):
        hot, values = [], [[] for _ in blocks[0][2]]
        for block, place, weights in blocks:
            hot.append(jnp.where(tile == place, 1.0, 0.0).astype(jnp.bfloat16))
            high = block.astype(jnp.bfloat16).astype(jnp.float32)
            both = jnp.concatenate([high, block - high], axis=0)
            for c, weight in enumerate(weights):
                values[c].append((both * weight).astype(jnp.bfloat16))
        left = jnp.concatenate([jnp.concatenate(v, axis=1) for v in values], axis=0)
        right = jnp.concatenate(hot, axis=1)
        return lax.dot_general(
            left, right, (((1,), (1,)), ((), ())), preferred_element_type=jnp.float32
        )

    def weights_of(block):
        return [mask[c, pl.ds(block, 1), :] for c in range(3)]

    def whole(block, weights):
        return block, block[20:21], weights

    acc[0:144] = jnp.zeros((144, CELLS), jnp.float32)

    def own_group(group, _):
        start = group * GROUP
        acc[0:144] += binned(
            [whole(own[start + k], weights_of(start + k)) for k in range(GROUP)]
        )
        return 0

    lax.fori_loop(0, LAG, own_group, 0)

    @pl.when(yields)
    def _():
        for copy in far_copies:
            copy.start()

    lax.fori_loop(LAG, BLOCKS // GROUP, own_group, 0)

    @pl.when(last_row)
    def _():
        pl.semaphore_wait(near_ok, 1)
        near_copy.start()

    near_copy.wait_recv()
    acc[0:144] += binned([whole(near_in[k], weights_of(near_id + k)) for k in range(CAP_X)])

    @pl.when(last_row)
    def _():
        pl.semaphore_wait(all_in, 1)
        for copy in note_copies:
            copy.start()

    for copy in note_copies:
        copy.wait_recv()
    slot = lax.broadcasted_iota(jnp.int32, (16, 128), 0)
    here = lax.broadcasted_iota(jnp.int32, (16, 128), 1) == slot + first_z
    far_named = named == (row + far_id).astype(jnp.float32)
    for kind in range(3):
        kinds = [note_in[side, kind : kind + 1, :] for side in range(2)]
        found = jnp.where(here, jnp.where(slot < CAP_Z, kinds[0], kinds[1]), 0.0)
        found = jnp.max(found, axis=1, keepdims=True)
        slot_mask[kind] = jnp.broadcast_to(found, (16, 128))
        for side in range(2):
            begin = first_z + CAP_Z * side
            inside = (spot >= begin) & (spot < begin + CAP_Z)
            found = jnp.where(far_named & inside, kinds[side], 0.0)
            found = jnp.max(found, axis=1, keepdims=True)
            far_mask[3 * side + kind] = jnp.broadcast_to(found, (8, 128))
    for side in range(2):
        blocks = []
        for k in range(CAP_Z):
            entry = lists[0, first_z + CAP_Z * side + k]
            place = entry - near_id
            valid = k < counts[0, 2 + side]
            valid = valid & ((entry < BLOCKS) | ((place >= 0) & (place < CAP_X)))
            block = own[jnp.clip(entry, 0, BLOCKS - 1)]
            other = near_in[jnp.clip(place, 0, CAP_X - 1)]
            block = jnp.where(valid, jnp.where(entry < BLOCKS, block, other), 0.0)
            at_slot = CAP_Z * side + k
            weights = [slot_mask[c, at_slot : at_slot + 1, :] for c in range(3)]
            blocks.append(whole(block, weights))
        acc[144 * (1 + side) : 144 * (2 + side)] = binned(blocks)

    @pl.when(gx == 0)
    def _():
        pl.semaphore_wait(ready, 1)
        for dz, dy in SENDS:
            pl.semaphore_signal(
                passed_on, inc=1, device_id=beside(gz=dz, gy=dy), device_id_type=MESH
            )

    @pl.when(early & (gx != 0))
    def _():
        pl.semaphore_wait(ready, 1)
        for copy in far_copies:
            copy.start()

    for pair, copy in enumerate(far_copies):
        copy.wait_recv()
        first = 1 + 5 * pair
        last = far_in[first + 4]
        blocks = []
        for k, top in ((2 * pair, last), (2 * pair + 1, pltpu.roll(last, 4, 0))):
            start = first + 2 * (k % 2)
            block = jnp.concatenate([far_in[start], far_in[start + 1], top], axis=0)
            weights = weights_of(far_id + k)
            weights += [far_mask[c, k : k + 1, :] for c in range(6)]
            blocks.append((block, far_in[0, k : k + 1, :], weights))
        acc[...] += binned(blocks)

    def packed(dz, dy):
        first = 144 * CLASS[dz] + 48 * CLASS[dy]
        sums = acc[first : first + 24] + acc[first + 24 : first + 48]
        tiles = [sums[8 * r : 8 * r + 8, 128 * k : 128 * k + 128] for r in (0, 1) for k in range(4)]
        for k in (0, 256):
            pair = [sums[16:20, k : k + 128], sums[16:20, k + 128 : k + 256]]
            tiles.append(jnp.concatenate(pair, axis=0))
        return tiles

    sum_copies = []
    for m, (dz, dy) in enumerate(SENDS):
        for k, part in enumerate(packed(dz, dy)):
            sum_send[m, k] = part
        sum_copies.append(
            remote(at + m, sum_send.at[m], sum_in.at[m], beside(gz=dz, gy=dy))
        )

    @pl.when(gx == 0)
    def _():
        for copy in far_copies:
            copy.start()
        pl.semaphore_wait(passed_on, len(SENDS))
        pl.semaphore_signal(
            all_in, inc=1, device_id=beside(gx=toward_far), device_id_type=MESH
        )

    result = packed(0, 0)
    for m, copy in enumerate(sum_copies):
        copy.wait_recv()
        result = [part + sum_in[m, k] for k, part in enumerate(result)]
    for k in range(4):
        columns = slice(128 * k, 128 * k + 128)
        out_ref[0:8, columns] = result[k]
        out_ref[8:16, columns] = result[4 + k]
        half = 4 * (k % 2)
        out_ref[16:20, columns] = result[8 + k // 2][half : half + 4]
    for copy in far_copies + [near_copy] + note_copies + sum_copies:
        copy.wait_send()


def solution(mesh):
    sizes = dict(mesh.shape)

    def per_device(particle_fields, step_length, live_mask, dest_cell, block_counts, block_lists):
        anywhere = pl.BlockSpec(memory_space=pl.ANY)
        copies = len(PARTS) + 3 + len(SENDS)
        return pl.pallas_call(
            functools.partial(kernel, sizes),
            out_shape=pltpu.VMEM((FIELDS, CELLS), jnp.float32),
            in_specs=[anywhere] * 6,
            out_specs=pl.BlockSpec(memory_space=pltpu.VMEM),
            scratch_shapes=[
                pltpu.VMEM((FIELDS, BLOCKS * 128), jnp.float32),
                pltpu.VMEM((BLOCKS, 128), jnp.float32),
                pltpu.VMEM((BLOCKS, 128), jnp.int32),
                pltpu.VMEM((BLOCKS, 128), jnp.int32),
                pltpu.SMEM((1, 6), jnp.int32),
                pltpu.SMEM((1, LIST_LEN), jnp.int32),
                pltpu.VMEM((1, LIST_LEN), jnp.int32),
                pltpu.VMEM((BLOCKS, ROWS, 128), jnp.float32),
                pltpu.VMEM((16, 8, 128), jnp.float32),
                pltpu.VMEM((CAP_X, ROWS, 128), jnp.float32),
                pltpu.VMEM((16, 8, 128), jnp.float32),
                pltpu.VMEM((CAP_X, ROWS, 128), jnp.float32),
                pltpu.VMEM((8, 128), jnp.float32),
                pltpu.VMEM((8, 128), jnp.float32),
                pltpu.VMEM((2, 8, 128), jnp.float32),
                pltpu.VMEM((len(SENDS), 10, 8, 128), jnp.float32),
                pltpu.VMEM((len(SENDS), 10, 8, 128), jnp.float32),
                pltpu.VMEM((3, BLOCKS + 16, 128), jnp.float32),
                pltpu.VMEM((6, 8, 128), jnp.float32),
                pltpu.VMEM((3, 16, 128), jnp.float32),
                pltpu.VMEM((9 * 2 * ROWS, CELLS), jnp.float32),
                pltpu.SemaphoreType.DMA((10,)),
                pltpu.SemaphoreType.DMA((copies,)),
                pltpu.SemaphoreType.DMA((copies,)),
                pltpu.SemaphoreType.REGULAR,
                pltpu.SemaphoreType.REGULAR,
                pltpu.SemaphoreType.REGULAR,
                pltpu.SemaphoreType.REGULAR,
            ],
            compiler_params=pltpu.CompilerParams(collective_id=0, has_side_effects=True),
        )(
            particle_fields,
            step_length.reshape(BLOCKS, 128),
            live_mask.reshape(BLOCKS, 128),
            dest_cell.reshape(BLOCKS, 128),
            block_counts,
            block_lists,
        )

    placed = (P(None, AXES), P(AXES), P(AXES), P(AXES), P(AXES, None), P(AXES, None))
    return jax.shard_map(
        per_device, mesh=mesh, in_specs=placed, out_specs=P(None, AXES), check_vma=False
    )
```
